256 devices in a mesh: dp: 4 (over y), expert: 64 (over z, x, core).
Axes of the slice: x: 4, y: 4, z: 8, core: 2. Of those that a mesh axis runs over, the one named last changes fastest.
Arguments:
- grad_out: bfloat16 [32768, 3072], P(('dp', 'expert')), may hold values from -6 to 6
- expert_ids: int32 [32768, 2], P(('dp', 'expert')), may hold values from 0 to 7, all different within a row; in each aligned block of 128 rows (0 to 127, 128 to 255, ...) at most 36 rows name the same one
- down_weight: bfloat16 [64, 1024, 3072], P('expert'), may hold values from -0.109375 to 0.109375
- history_grad: float32 [8, 8], replicated, may hold values from 0.5 to 3
- history_hidden: float32 [8, 8], replicated, may hold values from 0.5 to 3
Outputs:
- hidden_scaled: bfloat16 [4, 64, 2304, 1024], P('dp', 'expert')
- new_history_grad: float32 [8, 8], replicated
- new_history_hidden: float32 [8, 8], replicated
The draws below stay inside these ranges and needn't reach their ends.
Inputs may be any that keep to these rules, and one draw needn't show every extreme that they name: `expert_ids`: each row names 2 different experts; among the 128 rows of one device no expert is named more than 36 times, a bound that some block reaches in some devices.
All inputs are finite; a program needn't handle non-finite values.
Results may differ from the reference program's by a relative error of at most 0.0045.
Values may be sent and summed in bfloat16 or wider, within the bound.
A program may use at most 128 MiB of HBM per device.

```python
import math
import jax
import jax.numpy as jnp
import numpy as np
from jax import lax

D = 3072
EXPERTS = 8
TOP = 2
FF_DEV = 1024
HIST = 8
TOK_DEV = 128
CAP = 36
TOKENS = 32768
N_DP = 4
N_EXPERT = 64


def steps_of(key, dims, split, smallest, top_value):
    level, own = 1.0, jax.random.fold_in(key, 6)
    for axis_at, shards_of in split:
        steps = jnp.exp(jax.random.uniform(jax.random.fold_in(own, axis_at), (shards_of,), jnp.float32, smallest / len(split), top_value / len(split)))
        level = level * jnp.repeat(steps, dims[axis_at] // shards_of).reshape([-1 if axis == axis_at else 1 for axis in range(len(dims))])
    return level


def deal_out(own_key, own, number, rows, number_of, top, bound, lean):
    ranking = jax.random.permutation(own_key, number_of)
    packed, ordinary = portions_of(number_of, rows * top, bound, lean, True), portions_of(number_of, rows * top, bound, lean, False)
    places = jnp.arange(number_of)

    def named(lengths, turn):
        used = int((lengths > 0).sum())
        fixed = max(1, used // 4)
        moved = fixed + (places - fixed + turn * (used - fixed)) % max(1, number_of - fixed)
        return jnp.zeros((number_of,), jnp.int32).at[ranking[jnp.where(places < fixed, places, moved)]].set(jnp.asarray(lengths, jnp.int32))

    lengths = jnp.where(number % 4 == 0, named(packed, number // 4), named(ordinary, number - number // 4 - 1))
    mixed = jax.random.permutation(jax.random.fold_in(own, 3), number_of)
    giver, receiver = mixed[0:number_of // 2 * 2:2], mixed[1:number_of // 2 * 2:2]
    room = jnp.minimum(lengths[giver] - 1, bound - lengths[receiver]) // 2
    room = jnp.where((giver == ranking[0]) | (receiver == ranking[0]) | (lengths[receiver] == 0), 0, jnp.maximum(room, 0))
    moved = jax.random.randint(jax.random.fold_in(own, 4), (number_of // 2,), 0, 1 << 20) % (room + 1)
    lengths = lengths.at[giver].add(-moved).at[receiver].add(moved)
    items = jnp.searchsorted(jnp.cumsum(lengths), jnp.arange(rows * top), side="right").astype(jnp.int32)
    grid = items.reshape(top, rows).T
    grid = grid[jax.random.permutation(jax.random.fold_in(own, 1), rows)]
    turn = jax.random.randint(jax.random.fold_in(own, 2), (rows, 1), 0, top)
    return jnp.take_along_axis(grid, (jnp.arange(top)[None, :] + turn) % top, axis=1)


def portions_of(count, total, bound, slope, full):
    loads = [(1 << 20) // math.isqrt(rank ** slope) + 1 for rank in range(1, count + 1)]
    largest = bound if full else min(bound, max(-(-total // count), total * loads[0] // sum(loads)))
    least = 1 if total - largest >= count - 1 else 0
    given, surplus = [largest] + [least] * (count - 1), total - largest - least * (count - 1)
    while surplus > 0:
        candidates = [i for i in range(1, count) if given[i] < largest] or [i for i in range(1, count) if given[i] < bound]
        mass, budget = sum([loads[i] for i in candidates]), surplus
        for i in candidates:
            extra = min(bound - given[i], max(1, budget * loads[i] // mass), surplus)
            given[i] = given[i] + extra
            surplus = surplus - extra
    return np.array(given)


def centred(own_key, shape, spread, bound, split=(), held_as=jnp.bfloat16):
    result = jax.random.normal(own_key, shape, jnp.float32) * spread
    if len(split) > 0:
        result = steps_of(own_key, shape, split, -0.22, 0.18) * result
    return jnp.clip(result, min=-bound, max=bound).astype(held_as)


def setup_inputs(seed: int = 0) -> dict:
    seeds = jax.random.split(jax.random.key(seed), 6)
    grad_out = centred(seeds[0], (TOKENS, D), 1.0, 6.0, ((0, 256),))
    expert_ids_keys = jax.random.split(jax.random.fold_in(seeds[1], 1), TOKENS // TOK_DEV)
    expert_ids_turns = jax.random.permutation(jax.random.fold_in(seeds[1], 3), TOKENS // TOK_DEV)
    expert_ids = jax.vmap(lambda own, number: deal_out(jax.random.fold_in(seeds[1], 2), own, number, TOK_DEV, EXPERTS, TOP, CAP, 2))(expert_ids_keys, expert_ids_turns).reshape((TOKENS, TOP))
    down_weight = centred(seeds[2], (N_EXPERT, FF_DEV, D), D ** -0.5, 0.109375, ((0, 64),))
    history_grad = jnp.clip(jnp.exp(jax.random.uniform(seeds[3], (HIST, EXPERTS), jnp.float32, math.log(0.5), math.log(3.0))), 0.5, 3.0)
    history_hidden = jnp.clip(jnp.exp(jax.random.uniform(seeds[4], (HIST, EXPERTS), jnp.float32, math.log(0.5), math.log(3.0))), 0.5, 3.0)
    return {"grad_out": grad_out, "expert_ids": expert_ids, "down_weight": down_weight, "history_grad": history_grad, "history_hidden": history_hidden}


def reference(grad_out, expert_ids, down_weight, history_grad, history_hidden):
    slices = N_EXPERT // EXPERTS
    routing = expert_ids.reshape(N_DP, N_EXPERT, TOK_DEV * TOP)
    onehot = (routing[..., None] == jnp.arange(EXPERTS, dtype=jnp.int32)).astype(jnp.int32)
    before = jnp.cumsum(onehot, axis=2) - onehot
    slot_index = jnp.sum(before * onehot, axis=-1).astype(jnp.int32)
    scale_in = 1.0 / jnp.max(history_grad, axis=0)
    scale_hidden = 1.0 / jnp.max(history_hidden, axis=0)
    gradients = grad_out.reshape(N_DP, N_EXPERT, TOK_DEV, D)
    row_peak = jnp.max(jnp.abs(gradients.astype(jnp.float32)), axis=-1)
    routed = jnp.max(onehot.reshape(N_DP, N_EXPERT, TOK_DEV, TOP, EXPERTS), axis=3) > 0
    grad_amax = jnp.max(jnp.where(routed, row_peak[..., None], 0.0), axis=(0, 1, 2))
    token_of = jnp.arange(TOK_DEV * TOP, dtype=jnp.int32) // TOP
    weights = down_weight.reshape(EXPERTS, slices * FF_DEV, D)
    source_index = jnp.broadcast_to(jnp.arange(N_EXPERT, dtype=jnp.int32)[:, None], (N_EXPERT, TOK_DEV * TOP))

    def one_replica(inputs):
        grads_here, routing_here, slots_here = inputs
        token_rows = grads_here[:, token_of].astype(jnp.float32)
        quantized = jnp.clip(token_rows * scale_in[routing_here][..., None], -1.0, 1.0).astype(jnp.bfloat16)
        buffer = jnp.zeros((EXPERTS, N_EXPERT, CAP, D), jnp.bfloat16)
        buffer = buffer.at[routing_here, source_index, slots_here].set(quantized)

        def one_expert(pair):
            expert, block = pair
            received = block.reshape(N_EXPERT * CAP, D)
            product = jnp.dot(received, weights[expert].T, preferred_element_type=jnp.float32)
            hidden = product / scale_in[expert]
            scaled = jnp.clip(hidden * scale_hidden[expert], -1.0, 1.0).astype(jnp.bfloat16)
            scaled = scaled.reshape(N_EXPERT * CAP, slices, FF_DEV).transpose(1, 0, 2)
            return scaled, jnp.max(jnp.abs(hidden))

        scaled, peak_values = lax.map(one_expert, (jnp.arange(EXPERTS, dtype=jnp.int32), buffer))
        return scaled.reshape(N_EXPERT, N_EXPERT * CAP, FF_DEV), peak_values

    hidden_scaled, peak_values = lax.map(one_replica, (gradients, routing, slot_index))
    hidden_amax = jnp.max(peak_values, axis=0)
    new_history_grad = jnp.concatenate([history_grad[1:], grad_amax[None, :]], axis=0)
    new_history_hidden = jnp.concatenate([history_hidden[1:], hidden_amax[None, :]], axis=0)
    return hidden_scaled, new_history_grad, new_history_hidden
```

```python
import functools

import jax
import jax.numpy as jnp
from jax import lax
from jax.experimental import pallas as pl
from jax.experimental.pallas import tpu as pltpu
from jax.sharding import PartitionSpec as P

MESH = pl.DeviceIdType.MESH
F32, BF16 = jnp.float32, jnp.bfloat16
CORES = 2
MAIN = 32
UNITS = 256


def ceil_parts(values, width, count):
    return functools.reduce(lambda a, b: a + b, [(values >= width * i).astype(jnp.int32) for i in range(1, count)])


def kernel(
    n_y, n_z, n_x, capacity,
    ids_ref, hist_grad, hist_hidden, grad_hbm, weight_hbm,
    out_hbm, new_grad, new_hidden,
    grad_v, weight_v, queue, gathered, staged, slot_of, unfold, order, grad_peak, hidden_peak, message, inbox,
    local_sem, out_sem, z_send, z_recv, x_send, x_recv, f_send, f_recv, d_send, d_recv, m_send, m_recv,
):
    tok = grad_v.shape[0]
    features = grad_v.shape[1]
    tail = capacity - MAIN
    fold = MAIN // tail
    width = features // fold
    members = n_x * CORES
    rows = members * MAIN
    extra = members * tail
    n_units = weight_v.shape[0]

    y = lax.axis_index("dp")
    me = lax.axis_index("expert")
    core = me % CORES
    x = (me // CORES) % n_x
    z = me // members
    group = me % members

    def at(to_z, to_x, to_core):
        return (y, (to_z * n_x + to_x) * CORES + to_core)

    right, left, far = (x + 1) % n_x, (x + n_x - 1) % n_x, (x + 2) % n_x
    partner = at(z, x, 1 - core)

    peers = [
        [at(z, ((group + j) % members) // CORES, ((group + j) % members) % CORES) for j in range(1, members)],
        [((y + j) % n_y, me) for j in range(1, n_y)],
        [at((z + j) % n_z, x, core) for j in range(1, n_z)],
    ]
    barrier = pltpu.get_barrier_semaphore()
    for phase in peers:
        for peer in phase:
            pl.semaphore_signal(barrier, inc=1, device_id=peer, device_id_type=MESH)

    grad_in = pltpu.make_async_copy(grad_hbm, grad_v, local_sem.at[0])
    grad_in.start()
    weight_in = pltpu.make_async_copy(weight_hbm, weight_v, local_sem.at[1])
    weight_in.start()

    def iota(shape, axis):
        return lax.broadcasted_iota(jnp.int32, shape, axis)

    ids = ids_ref[...]
    named = (iota((n_z, tok), 0) == ids[0:1, :]) | (iota((n_z, tok), 0) == ids[1:2, :])
    earlier = (iota((tok, tok), 0) < iota((tok, tok), 1)).astype(F32).astype(BF16)
    before = jnp.dot(named.astype(F32).astype(BF16), earlier, preferred_element_type=F32)
    slot_of[...] = jnp.where(named, before, -1.0)

    scale_in = 1.0 / jnp.max(hist_grad[...], axis=0, keepdims=True)
    scale_hidden = 1.0 / jnp.max(hist_hidden[...], axis=0, keepdims=True)
    own = iota((1, n_z), 1) == z
    own_in = jnp.sum(jnp.where(own, scale_in, 0.0), axis=1, keepdims=True)
    own_hidden = jnp.sum(jnp.where(own, scale_hidden, 0.0), axis=1, keepdims=True)

    all_rows = n_z * MAIN
    slots = jnp.broadcast_to(slot_of[...][:, None, :], (n_z, MAIN, tok)).reshape(all_rows, tok)
    in_block = iota((all_rows, tok), 0) % MAIN
    pick_main = (slots == in_block.astype(F32)).astype(F32).astype(BF16)
    is_tail = slots == (in_block % tail + MAIN).astype(F32)
    row_scale = jnp.sum(
        jnp.where(iota((all_rows, n_z), 1) == iota((all_rows, n_z), 0) // MAIN, scale_in, 0.0), axis=1, keepdims=True
    )

    def scaled(values):
        return jnp.clip(values * row_scale, -1.0, 1.0).astype(BF16).reshape(n_z, MAIN, width)

    def folded_peak(values):
        return functools.reduce(jnp.maximum, [jnp.abs(values[:, i:i + 128]) for i in range(0, width, 128)])

    grad_in.wait()
    tails = jnp.zeros((all_rows, width), F32)
    peak = jnp.zeros((all_rows, 128), F32)
    for part in range(fold):
        piece = grad_v[:, part * width:(part + 1) * width]
        values = jnp.dot(pick_main, piece, preferred_element_type=F32)
        queue[:, :, part * width:(part + 1) * width] = scaled(values)
        peak = jnp.maximum(peak, folded_peak(values))
        pick = (is_tail & (in_block // tail == part)).astype(F32).astype(BF16)
        tails = tails + jnp.dot(pick, piece, preferred_element_type=F32)
    queue[:, :, features:] = scaled(tails)
    peak = jnp.maximum(peak, folded_peak(tails))
    peak = jnp.max(jnp.max(peak.reshape(n_z, MAIN, 128), axis=1), axis=1, keepdims=True)
    grad_peak[...] = jnp.broadcast_to(peak, (n_z, 128))
    hidden_peak[...] = jnp.zeros_like(hidden_peak)
    gathered[0, pl.ds(pl.multiple_of(group * MAIN, MAIN), MAIN), :] = queue[z]

    goes, comes = iota((rows, rows), 0), iota((rows, rows), 1)
    wanted = (goes % extra // tail) * MAIN + (goes // extra) * tail + goes % tail
    unfold[...] = (wanted == comes).astype(F32).astype(BF16)
    half = order.shape[0]
    goes, comes = iota((half, half), 0), iota((half, half), 1)
    block = ceil_parts(goes, capacity, members // 2)
    slot = goes - block * capacity
    wanted = jnp.where(slot < MAIN, block * MAIN + slot, rows // 2 + block * tail + slot - MAIN)
    order[...] = (wanted == comes).astype(F32).astype(BF16)

    pl.semaphore_wait(barrier, sum(len(phase) for phase in peers))

    def offset(k):
        return ((k + 1) // 2) * (2 * (k % 2) - 1)

    def part_of(k, member, low=0, count=MAIN):
        start = pl.multiple_of(member * MAIN + low, MAIN // 2)
        return gathered.at[k, pl.ds(start, count), :]

    def remote(source, target, send, recv, device):
        return pltpu.make_async_remote_copy(
            src_ref=source, dst_ref=target, send_sem=send, recv_sem=recv, device_id=device, device_id_type=MESH
        )

    def z_copy(k):
        to_z = (z - offset(k) + n_z) % n_z
        return remote(queue.at[to_z], part_of(k, group), z_send.at[k], z_recv.at[k], at(to_z, x, core))

    def x_copy(k, way):
        mine = part_of(k, group)
        return remote(mine, mine, x_send.at[k, way], x_recv.at[k, way], at(z, (right, left)[way], core))

    def x_arrival(k, way):
        theirs = part_of(k, (left, right)[way] * CORES + core)
        return remote(theirs, theirs, x_send.at[k, way], x_recv.at[k, way], partner)

    def f_copy(k, way):
        theirs = part_of(k, (left, right)[way] * CORES + core, way * (MAIN // 2), MAIN // 2)
        return remote(theirs, theirs, f_send.at[k, way], f_recv.at[k, way], at(z, (right, left)[way], core))

    def f_arrival(k, way):
        theirs = part_of(k, far * CORES + core, way * (MAIN // 2), MAIN // 2)
        return remote(theirs, theirs, f_send.at[k, way], f_recv.at[k, way], partner)

    def d_copy(k, piece, whose):
        if piece < 3:
            block = part_of(k, (x, left, right)[piece] * CORES + whose)
        else:
            block = part_of(k, far * CORES + whose, (piece - 3) * (MAIN // 2), MAIN // 2)
        return remote(block, block, d_send.at[k, piece], d_recv.at[k, piece], partner)

    def z_body(k, carry):
        z_copy(k).start()
        return carry

    lax.fori_loop(1, n_z, z_body, 0)
    weight_in.wait()

    factor = own_hidden / own_in

    def out_copy(k):
        from_z = (z + offset(k) + n_z) % n_z
        start = pl.multiple_of(from_z * (members * capacity), members * capacity)
        return pltpu.make_async_copy(
            staged.at[k % 2], out_hbm.at[0, 0, pl.ds(start, members * capacity), :], out_sem.at[k % 2]
        )

    def multiply(k):
        folded = gathered[k, 0:rows, features:features + width]
        plain = jnp.dot(unfold[...], folded, preferred_element_type=F32).astype(BF16)
        for part in range(fold):
            gathered[k, rows:rows + extra, part * width:(part + 1) * width] = plain[part * extra:(part + 1) * extra]

        @pl.when(k >= 2)
        def _():
            out_copy(k - 2).wait()

        def unit_body(n, carry):
            start = pl.multiple_of(n * UNITS, UNITS)
            product = lax.dot_general(
                gathered[k, :, 0:features], weight_v[pl.ds(start, UNITS), :],
                (((1,), (1,)), ((), ())), preferred_element_type=F32,
            )
            size = jnp.abs(product).reshape((rows + extra) // 8, 8, UNITS)
            hidden_peak[...] = jnp.maximum(hidden_peak[...], jnp.max(size, axis=0))
            result = jnp.clip(product * factor, -1.0, 1.0).astype(BF16)
            for side in range(2):
                low, low_extra = side * (rows // 2), rows + side * (extra // 2)
                picked = jnp.concatenate(
                    [result[low:low + rows // 2], result[low_extra:low_extra + extra // 2]], axis=0
                )
                ordered = jnp.dot(order[...], picked, preferred_element_type=F32).astype(BF16)
                staged[k % 2, side * half:(side + 1) * half, pl.ds(start, UNITS)] = ordered
            return carry

        lax.fori_loop(0, n_units // UNITS, unit_body, 0)
        out_copy(k).start()

    def step(i, carry):
        @pl.when((i >= 1) & (i < n_z))
        def _():
            z_copy(i).wait_recv()

        @pl.when(i < n_z)
        def _():
            x_copy(i, 0).start()
            x_copy(i, 1).start()
            d_copy(i, 0, core).start()

        @pl.when((i >= 1) & (i < n_z + 1))
        def _():
            k = i - 1
            for way in range(2):
                x_arrival(k, way).wait_recv()
                f_copy(k, way).start()
                d_copy(k, 1 + way, core).start()

        @pl.when(i >= 2)
        def _():
            k = i - 2
            for way in range(2):
                f_arrival(k, way).wait_recv()
                d_copy(k, 3 + way, core).start()
            for piece in range(5):
                d_copy(k, piece, 1 - core).wait_recv()
            multiply(k)

        return carry

    lax.fori_loop(0, n_z + 2, step, 0)

    hidden_max = jnp.max(jnp.max(hidden_peak[...], axis=0, keepdims=True), axis=1, keepdims=True) / own_in
    hidden_rows = jnp.where(iota((n_z, 128), 0) == z, hidden_max, 0.0)
    current = jnp.concatenate([grad_peak[...], hidden_rows], axis=0)
    base = 0
    for turn, phase in enumerate(peers):
        message[turn] = current
        for j, peer in enumerate(phase):
            remote(message.at[turn], inbox.at[base + j], m_send.at[base + j], m_recv.at[base + j], peer).start()
        for j, peer in enumerate(phase):
            remote(message.at[turn], inbox.at[base + j], m_send.at[base + j], m_recv.at[base + j], peer).wait_recv()
            current = jnp.maximum(current, inbox[base + j])
        base += len(phase)

    def history(old, peaks):
        diagonal = jnp.where(iota((n_z, 128), 0) == iota((n_z, 128), 1), peaks, 0.0)
        newest = jnp.max(diagonal, axis=0, keepdims=True)[:, 0:n_z]
        return jnp.concatenate([old[1:], newest], axis=0)

    new_grad[...] = history(hist_grad[...], current[0:n_z])
    new_hidden[...] = history(hist_hidden[...], current[n_z:2 * n_z])

    out_copy(n_z - 2).wait()
    out_copy(n_z - 1).wait()

    def drain(k, carry):
        @pl.when(k >= 1)
        def _():
            z_copy(k).wait_send()

        for way in range(2):
            x_copy(k, way).wait_send()
            f_copy(k, way).wait_send()
        for piece in range(5):
            d_copy(k, piece, core).wait_send()
        return carry

    lax.fori_loop(0, n_z, drain, 0)
    base = 0
    for turn, phase in enumerate(peers):
        for j, peer in enumerate(phase):
            remote(message.at[turn], inbox.at[base + j], m_send.at[base + j], m_recv.at[base + j], peer).wait_send()
        base += len(phase)


def solution(mesh):
    n_y = mesh.shape["dp"]
    n_expert = mesh.shape["expert"]

    def per_device(grad_out, expert_ids, down_weight, history_grad, history_hidden):
        tok, features = grad_out.shape
        n_z = history_grad.shape[1]
        members = n_expert // n_z
        n_x = members // CORES
        units = down_weight.shape[1]
        capacity = tok * 9 // 32
        tail = capacity - MAIN
        width = features * tail // MAIN
        rows, extra = members * MAIN, members * tail
        n_messages = members - 1 + n_y - 1 + n_z - 1
        dma = pltpu.SemaphoreType.DMA
        vmem, anywhere = pl.BlockSpec(memory_space=pltpu.VMEM), pl.BlockSpec(memory_space=pl.ANY)
        small = jax.ShapeDtypeStruct(history_grad.shape, F32)
        return pl.pallas_call(
            functools.partial(kernel, n_y, n_z, n_x, capacity),
            out_shape=(jax.ShapeDtypeStruct((1, 1, n_expert * capacity, units), BF16), small, small),
            in_specs=[vmem, vmem, vmem, anywhere, anywhere],
            out_specs=(anywhere, vmem, vmem),
            scratch_shapes=[
                pltpu.VMEM((tok, features), BF16),
                pltpu.VMEM((units, features), BF16),
                pltpu.VMEM((n_z, MAIN, features + width), BF16),
                pltpu.VMEM((n_z, rows + extra, features + width), BF16),
                pltpu.VMEM((2, members * capacity, units), BF16),
                pltpu.VMEM((n_z, tok), F32),
                pltpu.VMEM((rows, rows), BF16),
                pltpu.VMEM((members * capacity // 2, members * capacity // 2), BF16),
                pltpu.VMEM((n_z, 128), F32),
                pltpu.VMEM((8, UNITS), F32),
                pltpu.VMEM((3, 2 * n_z, 128), F32),
                pltpu.VMEM((n_messages, 2 * n_z, 128), F32),
                dma((2,)), dma((2,)),
                dma((n_z,)), dma((n_z,)),
                dma((n_z, 2)), dma((n_z, 2)),
                dma((n_z, 2)), dma((n_z, 2)),
                dma((n_z, 5)), dma((n_z, 5)),
                dma((n_messages,)), dma((n_messages,)),
            ],
            compiler_params=pltpu.CompilerParams(
                collective_id=0, has_side_effects=True, vmem_limit_bytes=60 * 1024 * 1024
            ),
        )(expert_ids.T, history_grad, history_hidden, grad_out, down_weight[0])

    both = ("dp", "expert")
    return jax.shard_map(
        per_device,
        mesh=mesh,
        in_specs=(P(both, None), P(both, None), P("expert", None, None), P(), P()),
        out_specs=(P("dp", "expert", None, None), P(), P()),
        check_vma=False,
    )
```

```python
import functools

import jax
import jax.numpy as jnp
from jax import lax
from jax.experimental import pallas as pl
from jax.experimental.pallas import tpu as pltpu
from jax.sharding import PartitionSpec as P

MESH = pl.DeviceIdType.MESH
F32, BF16 = jnp.float32, jnp.bfloat16
CORES = 2
MAIN = 32
HALF = MAIN // 2
PAIR = CORES * MAIN
NEAR = 3 * PAIR
FAR = NEAR + 32
FAR_ROWS = PAIR + 16


def iota(shape, axis):
    return lax.broadcasted_iota(jnp.int32, shape, axis)


def unfold_matrix(rows, tail, fold):
    extra = rows // MAIN * tail
    goes, comes = iota((rows, rows), 0), iota((rows, rows), 1)
    part = functools.reduce(lambda a, b: a + b, [(goes >= extra * i).astype(jnp.int32) for i in range(1, fold)])
    rest = goes - part * extra
    wanted = rest // tail * MAIN + part * tail + rest % tail
    return (wanted == comes).astype(F32).astype(BF16)


def kernel(
    n_y, n_z, n_x, capacity,
    ids_hbm, hist_grad_hbm, hist_hidden_hbm, grad_hbm, weight_hbm,
    out_ref, new_grad, new_hidden,
    ids_ref, hist_grad, hist_hidden, grad_v, weight_v, queue, gathered, slot_of, unfold_near, unfold_far, peaks, hidden_peak, message, inbox,
    local_sem, z_send, z_recv, x_send, x_recv, f_send, f_recv, d_send, d_recv, m_send, m_recv,
):
    tok, features = grad_v.shape
    units = weight_v.shape[0]
    tail = capacity - MAIN
    fold = MAIN // tail
    width = features // fold
    members = n_x * CORES

    y = lax.axis_index("dp")
    me = lax.axis_index("expert")
    core = me % CORES
    x = (me // CORES) % n_x
    z = me // members
    group = me % members

    def at(to_z, to_x, to_core):
        return (y, (to_z * n_x + to_x) * CORES + to_core)

    right, left, far = (x + 1) % n_x, (x + n_x - 1) % n_x, (x + 2) % n_x
    partner = at(z, x, 1 - core)
    sides = (at(z, right, core), at(z, left, core))

    peers = [
        [
            ((y + i) % n_y, z * members + (group + j) % members)
            for i in range(n_y) for j in range(members) if i + j > 0
        ],
        [at((z + j) % n_z, x, core) for j in range(1, n_z)],
    ]
    barrier = pltpu.get_barrier_semaphore()
    for phase in peers[::-1]:
        for peer in phase:
            pl.semaphore_signal(barrier, inc=1, device_id=peer, device_id_type=MESH)

    pairs = (ids_hbm, ids_ref), (hist_grad_hbm, hist_grad), (hist_hidden_hbm, hist_hidden), (grad_hbm, grad_v), (weight_hbm, weight_v)
    loads = [pltpu.make_async_copy(source, target, local_sem.at[i]) for i, (source, target) in enumerate(pairs)]
    for load in loads:
        load.start()
    grad_in, weight_in = loads[3:]
    for load in loads[:3]:
        load.wait()

    ids = ids_ref[...]
    named = (iota((n_z, tok), 0) == ids[0:1, :]) | (iota((n_z, tok), 0) == ids[1:2, :])
    earlier = (iota((tok, tok), 0) < iota((tok, tok), 1)).astype(F32).astype(BF16)
    before = jnp.dot(named.astype(F32).astype(BF16), earlier, preferred_element_type=F32)
    slot_of[...] = jnp.where(named, before, -1.0)

    scale_in = 1.0 / jnp.max(hist_grad[...], axis=0, keepdims=True)
    scale_hidden = 1.0 / jnp.max(hist_hidden[...], axis=0, keepdims=True)
    own = iota((1, n_z), 1) == z
    own_in = jnp.sum(jnp.where(own, scale_in, 0.0), axis=1, keepdims=True)
    own_hidden = jnp.sum(jnp.where(own, scale_hidden, 0.0), axis=1, keepdims=True)
    factor = own_hidden / own_in

    all_rows = n_z * MAIN
    slots = jnp.broadcast_to(slot_of[...][:, None, :], (n_z, MAIN, tok)).reshape(all_rows, tok)
    in_block = iota((all_rows, tok), 0) % MAIN
    pick_main = (slots == in_block.astype(F32)).astype(F32).astype(BF16)
    is_tail = slots == (in_block % tail + MAIN).astype(F32)
    row_scale = jnp.sum(
        jnp.where(iota((all_rows, n_z), 1) == iota((all_rows, n_z), 0) // MAIN, scale_in, 0.0), axis=1, keepdims=True
    )

    def scaled(values):
        return jnp.clip(values * row_scale, -1.0, 1.0).astype(BF16).reshape(n_z, MAIN, width)

    def folded_peak(values):
        return functools.reduce(jnp.maximum, [jnp.abs(values[:, i:i + 128]) for i in range(0, width, 128)])

    grad_in.wait()
    tails = jnp.zeros((all_rows, width), F32)
    peak = jnp.zeros((all_rows, 128), F32)
    for part in range(fold):
        piece = grad_v[:, part * width:(part + 1) * width]
        values = jnp.dot(pick_main, piece, preferred_element_type=F32)
        queue[:, :, part * width:(part + 1) * width] = scaled(values)
        peak = jnp.maximum(peak, folded_peak(values))
        pick = (is_tail & (in_block // tail == part)).astype(F32).astype(BF16)
        tails = tails + jnp.dot(pick, piece, preferred_element_type=F32)
    queue[:, :, features:] = scaled(tails)
    peak = jnp.maximum(peak, folded_peak(tails))
    peak = jnp.max(jnp.max(peak.reshape(n_z, MAIN, 128), axis=1), axis=1, keepdims=True)
    diagonal = jnp.where(iota((n_z, 128), 0) == iota((n_z, 128), 1), peak, 0.0)
    peaks[...] = jnp.max(diagonal, axis=0, keepdims=True)
    hidden_peak[...] = jnp.zeros_like(hidden_peak)
    gathered[0, pl.ds(pl.multiple_of(core * MAIN, MAIN), MAIN), :] = queue[z]
    unfold_near[...] = unfold_matrix(NEAR, tail, fold)
    unfold_far[...] = unfold_matrix(PAIR, tail, fold)

    pl.semaphore_wait(barrier, sum(len(phase) for phase in peers))

    starts = (0, PAIR, 2 * PAIR, FAR)

    def offset(k):
        return ((k + 1) // 2) * (2 * (k % 2) - 1)

    def part_of(k, place, whose, low=0, count=MAIN):
        start = pl.multiple_of(starts[place] + whose * MAIN + low, HALF)
        return gathered.at[k, pl.ds(start, count), :]

    def remote(source, target, send, recv, device):
        return pltpu.make_async_remote_copy(
            src_ref=source, dst_ref=target, send_sem=send, recv_sem=recv, device_id=device, device_id_type=MESH
        )

    def z_copy(k):
        to_z = (z - offset(k) + n_z) % n_z
        return remote(queue.at[to_z], part_of(k, 0, core), z_send.at[k], z_recv.at[k], at(to_z, x, core))

    def x_copy(k, way):
        return remote(
            part_of(k, 0, core), part_of(k, 1 + way, core), x_send.at[k, way], x_recv.at[k, way], sides[way]
        )

    def f_copy(k, way):
        return remote(
            part_of(k, 1 + way, core, way * HALF, HALF), part_of(k, 3, core, way * HALF, HALF),
            f_send.at[k, way], f_recv.at[k, way], sides[way],
        )

    def d_copy(k, piece, whose):
        if piece < 3:
            block = part_of(k, piece, whose)
        else:
            block = part_of(k, 3, whose, (piece - 3) * HALF, HALF)
        return remote(block, block, d_send.at[k, piece], d_recv.at[k, piece], partner)

    def pass_far(k):
        for way in range(2):
            f_copy(k, way).wait_recv()
            d_copy(k, 3 + way, core).start()

    def place_tails(k, low, rows, unfold):
        extra = rows // MAIN * tail
        room = -(-extra // 16) * 16
        folded = gathered[k, low:low + rows, features:features + width]
        plain = jnp.dot(unfold[...], folded, preferred_element_type=F32)
        for part in range(fold):
            piece = plain[part * extra:(part + 1) * extra]
            piece = jnp.concatenate([piece, jnp.zeros((room - extra, width), F32)], axis=0).astype(BF16)
            gathered[k, low + rows:low + rows + room, part * width:(part + 1) * width] = piece

    def multiply(k, low, rows, places, first, count):
        product = lax.dot_general(
            gathered[k, low:low + rows, 0:features], weight_v[first:first + count, :],
            (((1,), (1,)), ((), ())), preferred_element_type=F32,
        )
        size = jnp.max(jnp.abs(product).reshape(rows // 8, 8, count), axis=0)
        size = functools.reduce(jnp.maximum, [size[:, i:i + 128] for i in range(0, count, 128)])
        hidden_peak[...] = jnp.maximum(hidden_peak[...], size)
        result = jnp.clip(product * factor, -1.0, 1.0)
        from_z = (z + offset(k) + n_z) % n_z
        for place in places:
            start = starts[place] - low
            last = (NEAR + place * CORES * tail if place < 3 else FAR + PAIR) - low
            pieces = []
            for member in range(CORES):
                pieces.append(result[start + member * MAIN:start + (member + 1) * MAIN])
                pieces.append(result[last + member * tail:last + (member + 1) * tail])
            ordered = jnp.concatenate(pieces, axis=0).astype(BF16)
            out_ref[from_z * n_x + (x, left, right, far)[place], :, first:first + count] = ordered

    def near_ready(k):
        for piece in range(3):
            d_copy(k, piece, 1 - core).wait_recv()
        place_tails(k, 0, NEAR, unfold_near)

    def far_ready(k):
        for piece in range(3, 5):
            d_copy(k, piece, 1 - core).wait_recv()
        place_tails(k, FAR, PAIR, unfold_far)

    def send_own(k):
        x_copy(k, 0).start()
        x_copy(k, 1).start()
        d_copy(k, 0, core).start()

    def z_body(k, carry):
        z_copy(k).start()
        return carry

    send_own(0)
    lax.fori_loop(1, n_z, z_body, 0)
    weight_in.wait()

    last = n_z - 1

    def step(i, carry):
        @pl.when(i < last)
        def _():
            z_copy(i + 1).wait_recv()
            send_own(i + 1)

        @pl.when(i >= 2)
        def _():
            k = i - 2
            pass_far(k)
            near_ready(k)
            far_ready(k)
            multiply(k, 0, FAR + FAR_ROWS, (0, 1, 2, 3), 0, units)

        for way in range(2):
            x_copy(i, way).wait_recv()
            f_copy(i, way).start()
            d_copy(i, 1 + way, core).start()
        return carry

    lax.fori_loop(0, n_z, step, 0)
    near_ready(last)
    multiply(last, 0, FAR, (0, 1, 2), 0, units // 2)
    pass_far(last - 1)
    multiply(last, 0, FAR, (0, 1, 2), units // 2, units // 2)
    near_ready(last - 1)
    far_ready(last - 1)
    multiply(last - 1, 0, FAR + FAR_ROWS, (0, 1, 2, 3), 0, units // 2)
    pass_far(last)
    multiply(last - 1, 0, FAR + FAR_ROWS, (0, 1, 2, 3), units // 2, units // 2)
    far_ready(last)
    multiply(last, FAR, FAR_ROWS, (3,), 0, units)

    hidden_max = jnp.max(jnp.max(hidden_peak[...], axis=0, keepdims=True), axis=1, keepdims=True) / own_in
    hidden_row = jnp.where(iota((1, 128), 1) == z, hidden_max, 0.0)
    current = jnp.where(iota((2, 128), 0) == 0, peaks[...], hidden_row)
    base = 0
    for turn, phase in enumerate(peers):
        message[turn] = current
        for j, peer in enumerate(phase):
            remote(message.at[turn], inbox.at[base + j], m_send.at[base + j], m_recv.at[base + j], peer).start()
        for j, peer in enumerate(phase):
            remote(message.at[turn], inbox.at[base + j], m_send.at[base + j], m_recv.at[base + j], peer).wait_recv()
            current = jnp.maximum(current, inbox[base + j])
        base += len(phase)

    new_grad[...] = jnp.concatenate([hist_grad[...][1:], current[0:1, 0:n_z]], axis=0)
    new_hidden[...] = jnp.concatenate([hist_hidden[...][1:], current[1:2, 0:n_z]], axis=0)

    def drain(k, carry):
        @pl.when(k >= 1)
        def _():
            z_copy(k).wait_send()

        for way in range(2):
            x_copy(k, way).wait_send()
            f_copy(k, way).wait_send()
        for piece in range(5):
            d_copy(k, piece, core).wait_send()
        return carry

    lax.fori_loop(0, n_z, drain, 0)
    base = 0
    for turn, phase in enumerate(peers):
        for j, peer in enumerate(phase):
            remote(message.at[turn], inbox.at[base + j], m_send.at[base + j], m_recv.at[base + j], peer).wait_send()
        base += len(phase)


def solution(mesh):
    n_y = mesh.shape["dp"]
    n_expert = mesh.shape["expert"]

    def per_device(grad_out, expert_ids, down_weight, history_grad, history_hidden):
        tok, features = grad_out.shape
        n_z = history_grad.shape[1]
        members = n_expert // n_z
        n_x = members // CORES
        units = down_weight.shape[1]
        capacity = tok * 9 // 32
        width = features * (capacity - MAIN) // MAIN
        n_messages = n_y * members - 1 + n_z - 1
        dma = pltpu.SemaphoreType.DMA
        vmem, hbm = pl.BlockSpec(memory_space=pltpu.VMEM), pl.BlockSpec(memory_space=pltpu.HBM)
        small = jax.ShapeDtypeStruct(history_grad.shape, F32)
        arguments = expert_ids.T, history_grad, history_hidden, grad_out, down_weight[0]
        rows, new_grad, new_hidden = pl.pallas_call(
            functools.partial(kernel, n_y, n_z, n_x, capacity),
            out_shape=(jax.ShapeDtypeStruct((n_expert // CORES, CORES * capacity, units), BF16), small, small),
            in_specs=[hbm] * 5,
            out_specs=(vmem, vmem, vmem),
            scratch_shapes=[
                pltpu.VMEM((2, tok), jnp.int32),
                pltpu.VMEM(history_grad.shape, F32),
                pltpu.VMEM(history_grad.shape, F32),
                pltpu.VMEM((tok, features), BF16),
                pltpu.VMEM((units, features), BF16),
                pltpu.VMEM((n_z, MAIN, features + width), BF16),
                pltpu.VMEM((n_z, FAR + FAR_ROWS, features + width), BF16),
                pltpu.VMEM((n_z, tok), F32),
                pltpu.VMEM((NEAR, NEAR), BF16),
                pltpu.VMEM((PAIR, PAIR), BF16),
                pltpu.VMEM((1, 128), F32),
                pltpu.VMEM((8, 128), F32),
                pltpu.VMEM((2, 2, 128), F32),
                pltpu.VMEM((n_messages, 2, 128), F32),
                dma((5,)),
                dma((n_z,)), dma((n_z,)),
                dma((n_z, 2)), dma((n_z, 2)),
                dma((n_z, 2)), dma((n_z, 2)),
                dma((n_z, 5)), dma((n_z, 5)),
                dma((n_messages,)), dma((n_messages,)),
            ],
            compiler_params=pltpu.CompilerParams(
                collective_id=0, has_side_effects=True, vmem_limit_bytes=46 * 1024 * 1024
            ),
        )(*(pltpu.with_memory_space_constraint(a, pltpu.HBM) for a in arguments))
        return rows.reshape(1, 1, n_expert * capacity, units), new_grad, new_hidden

    both = ("dp", "expert")
    return jax.shard_map(
        per_device,
        mesh=mesh,
        in_specs=(P(both, None), P(both, None), P("expert", None, None), P(), P()),
        out_specs=(P("dp", "expert", None, None), P(), P()),
        check_vma=False,
    )
```

```python
import functools

import jax
import jax.numpy as jnp
from jax import lax
from jax.experimental import pallas as pl
from jax.experimental.pallas import tpu as pltpu
from jax.sharding import PartitionSpec as P

MESH = pl.DeviceIdType.MESH
F32, BF16 = jnp.float32, jnp.bfloat16
CORES = 2
MAIN = 32
HALF = MAIN // 2
PAIR = CORES * MAIN
NEAR = 3 * PAIR
FAR = NEAR + 32
FAR_ROWS = PAIR + 16
PIECES = 8


def iota(shape, axis):
    return lax.broadcasted_iota(jnp.int32, shape, axis)


def unfold_matrix(rows, tail, fold):
    extra = rows // MAIN * tail
    goes, comes = iota((rows, rows), 0), iota((rows, rows), 1)
    part = functools.reduce(lambda a, b: a + b, [(goes >= extra * i).astype(jnp.int32) for i in range(1, fold)])
    rest = goes - part * extra
    wanted = rest // tail * MAIN + part * tail + rest % tail
    return (wanted == comes).astype(F32).astype(BF16)


def kernel(
    n_y, n_z, n_x, capacity,
    ids_hbm, hist_grad_hbm, hist_hidden_hbm, grad_hbm, weight_hbm,
    out_ref, new_grad, new_hidden,
    ids_ref, hist_grad, hist_hidden, grad_v, weight_v, queue, gathered, slot_of, unfold_near, unfold_far, peaks, hidden_peak, message, inbox,
    local_sem, z_send, z_recv, o_send, o_recv, x_send, x_recv, f_send, f_recv, d_send, d_recv, m_send, m_recv,
):
    tok, features = grad_v.shape
    units = weight_v.shape[0]
    tail = capacity - MAIN
    fold = MAIN // tail
    width = features // fold
    members = n_x * CORES

    y = lax.axis_index("dp")
    me = lax.axis_index("expert")
    core = me % CORES
    x = (me // CORES) % n_x
    z = me // members
    group = me % members

    def at(to_z, to_x, to_core):
        return (y, (to_z * n_x + to_x) * CORES + to_core)

    right, left, far = (x + 1) % n_x, (x + n_x - 1) % n_x, (x + 2) % n_x
    partner = at(z, x, 1 - core)
    sides = (at(z, right, core), at(z, left, core))

    peers = [
        [
            ((y + i) % n_y, z * members + (group + j) % members)
            for i in range(n_y) for j in range(members) if i + j > 0
        ],
        [at((z + j) % n_z, x, core) for j in range(1, n_z)],
    ]
    barrier = pltpu.get_barrier_semaphore()
    for phase in peers[::-1]:
        for peer in phase:
            pl.semaphore_signal(barrier, inc=1, device_id=peer, device_id_type=MESH)

    pairs = (ids_hbm, ids_ref), (hist_grad_hbm, hist_grad), (hist_hidden_hbm, hist_hidden), (grad_hbm, grad_v), (weight_hbm, weight_v)
    loads = [pltpu.make_async_copy(source, target, local_sem.at[i]) for i, (source, target) in enumerate(pairs)]
    for load in loads:
        load.start()
    grad_in, weight_in = loads[3:]
    for load in loads[:3]:
        load.wait()

    ids = ids_ref[...]
    named = (iota((n_z, tok), 0) == ids[0:1, :]) | (iota((n_z, tok), 0) == ids[1:2, :])
    earlier = (iota((tok, tok), 0) < iota((tok, tok), 1)).astype(F32).astype(BF16)
    before = jnp.dot(named.astype(F32).astype(BF16), earlier, preferred_element_type=F32)
    slot_of[...] = jnp.where(named, before, -1.0)

    scale_in = 1.0 / jnp.max(hist_grad[...], axis=0, keepdims=True)
    scale_hidden = 1.0 / jnp.max(hist_hidden[...], axis=0, keepdims=True)
    own = iota((1, n_z), 1) == z
    own_in = jnp.sum(jnp.where(own, scale_in, 0.0), axis=1, keepdims=True)
    own_hidden = jnp.sum(jnp.where(own, scale_hidden, 0.0), axis=1, keepdims=True)
    factor = own_hidden / own_in

    all_rows = n_z * MAIN
    slots = jnp.broadcast_to(slot_of[...][:, None, :], (n_z, MAIN, tok)).reshape(all_rows, tok)
    in_block = iota((all_rows, tok), 0) % MAIN
    pick_main = (slots == in_block.astype(F32)).astype(F32).astype(BF16)
    is_tail = slots == (in_block % tail + MAIN).astype(F32)
    row_scale = jnp.sum(
        jnp.where(iota((all_rows, n_z), 1) == iota((all_rows, n_z), 0) // MAIN, scale_in, 0.0), axis=1, keepdims=True
    )

    def scaled(values):
        return jnp.clip(values * row_scale, -1.0, 1.0).astype(BF16).reshape(n_z, MAIN, width)

    def folded_peak(values):
        return functools.reduce(jnp.maximum, [jnp.abs(values[:, i:i + 128]) for i in range(0, width, 128)])

    grad_in.wait()
    tails = jnp.zeros((all_rows, width), F32)
    peak = jnp.zeros((all_rows, 128), F32)
    for part in range(fold):
        piece = grad_v[:, part * width:(part + 1) * width]
        values = jnp.dot(pick_main, piece, preferred_element_type=F32)
        queue[:, :, part * width:(part + 1) * width] = scaled(values)
        peak = jnp.maximum(peak, folded_peak(values))
        pick = (is_tail & (in_block // tail == part)).astype(F32).astype(BF16)
        tails = tails + jnp.dot(pick, piece, preferred_element_type=F32)
    queue[:, :, features:] = scaled(tails)
    peak = jnp.maximum(peak, folded_peak(tails))
    peak = jnp.max(jnp.max(peak.reshape(n_z, MAIN, 128), axis=1), axis=1, keepdims=True)
    diagonal = jnp.where(iota((n_z, 128), 0) == iota((n_z, 128), 1), peak, 0.0)
    peaks[...] = jnp.max(diagonal, axis=0, keepdims=True)
    hidden_peak[...] = jnp.zeros_like(hidden_peak)
    gathered[0, pl.ds(pl.multiple_of(core * MAIN, MAIN), MAIN), :] = queue[z]
    unfold_near[...] = unfold_matrix(NEAR, tail, fold)
    unfold_far[...] = unfold_matrix(PAIR, tail, fold)

    pl.semaphore_wait(barrier, sum(len(phase) for phase in peers))

    starts = (0, PAIR, 2 * PAIR, FAR)

    def offset(k):
        return ((k + 1) // 2) * (2 * (k % 2) - 1)

    def part_of(k, place, whose, low=0, count=MAIN):
        start = pl.multiple_of(starts[place] + whose * MAIN + low, HALF)
        return gathered.at[k, pl.ds(start, count), :]

    def remote(source, target, send, recv, device):
        return pltpu.make_async_remote_copy(
            src_ref=source, dst_ref=target, send_sem=send, recv_sem=recv, device_id=device, device_id_type=MESH
        )

    def z_copy(k):
        to_z = (z - offset(k) + n_z) % n_z
        return remote(queue.at[to_z], part_of(k, 0, core), z_send.at[k], z_recv.at[k], at(to_z, x, core))

    def x_copy(k, way):
        return remote(
            part_of(k, 0, core), part_of(k, 1 + way, core), x_send.at[k, way], x_recv.at[k, way], sides[way]
        )

    def first_copy(way, late):
        low = HALF * (way ^ late)
        return remote(
            part_of(0, 0, core, low, HALF), part_of(0, 1 + way, core, low, HALF),
            o_send.at[way, late], o_recv.at[way, late], sides[way],
        )

    def f_copy(k, way):
        return remote(
            part_of(k, 1 + way, core, way * HALF, HALF), part_of(k, 3, core, way * HALF, HALF),
            f_send.at[k, way], f_recv.at[k, way], sides[way],
        )

    def d_copy(k, piece, whose):
        if piece < 3:
            block = part_of(k, piece, whose)
        else:
            block = part_of(k, 3, whose, (piece - 3) * HALF, HALF)
        return remote(block, block, d_send.at[k, piece], d_recv.at[k, piece], partner)

    def pass_far(k):
        for way in range(2):
            f_copy(k, way).wait_recv()
            d_copy(k, 3 + way, core).start()

    def place_tails(k, low, rows, unfold):
        extra = rows // MAIN * tail
        room = -(-extra // 16) * 16
        folded = gathered[k, low:low + rows, features:features + width]
        plain = jnp.dot(unfold[...], folded, preferred_element_type=F32)
        for part in range(fold):
            piece = plain[part * extra:(part + 1) * extra]
            piece = jnp.concatenate([piece, jnp.zeros((room - extra, width), F32)], axis=0).astype(BF16)
            gathered[k, low + rows:low + rows + room, part * width:(part + 1) * width] = piece

    def multiply(k, low, rows, places, first, count):
        product = lax.dot_general(
            gathered[k, low:low + rows, 0:features], weight_v[first:first + count, :],
            (((1,), (1,)), ((), ())), preferred_element_type=F32,
        )
        size = jnp.max(jnp.abs(product).reshape(rows // 8, 8, count), axis=0)
        size = functools.reduce(jnp.maximum, [size[:, i:i + 128] for i in range(0, count, 128)])
        hidden_peak[...] = jnp.maximum(hidden_peak[...], size)
        result = jnp.clip(product * factor, -1.0, 1.0)
        from_z = (z + offset(k) + n_z) % n_z
        for place in places:
            start = starts[place] - low
            last = (NEAR + place * CORES * tail if place < 3 else FAR + PAIR) - low
            pieces = []
            for member in range(CORES):
                pieces.append(result[start + member * MAIN:start + (member + 1) * MAIN])
                pieces.append(result[last + member * tail:last + (member + 1) * tail])
            ordered = jnp.concatenate(pieces, axis=0).astype(BF16)
            out_ref[from_z * n_x + (x, left, right, far)[place], :, first:first + count] = ordered

    def near_ready(k):
        for piece in range(3):
            d_copy(k, piece, 1 - core).wait_recv()
        place_tails(k, 0, NEAR, unfold_near)

    def far_ready(k):
        for piece in range(3, 5):
            d_copy(k, piece, 1 - core).wait_recv()
        place_tails(k, FAR, PAIR, unfold_far)

    def send_own(k):
        x_copy(k, 0).start()
        x_copy(k, 1).start()
        d_copy(k, 0, core).start()

    def z_body(k, carry):
        z_copy(k).start()
        return carry

    for late in range(2):
        for way in range(2):
            first_copy(way, late).start()
    lax.fori_loop(1, n_z, z_body, 0)
    d_copy(0, 0, core).start()
    weight_in.wait()

    last = n_z - 1

    def step(i, carry):
        @pl.when(i < last)
        def _():
            z_copy(i + 1).wait_recv()
            send_own(i + 1)

        @pl.when(i >= 2)
        def _():
            k = i - 2
            pass_far(k)
            near_ready(k)
            far_ready(k)
            multiply(k, 0, FAR + FAR_ROWS, (0, 1, 2, 3), 0, units)

        for way in range(2):
            x_copy(i, way).wait_recv()
            f_copy(i, way).start()
            d_copy(i, 1 + way, core).start()
        return carry

    for way in range(2):
        first_copy(way, 0).wait_recv()
        f_copy(0, way).start()
    z_copy(1).wait_recv()
    send_own(1)
    for way in range(2):
        first_copy(way, 1).wait_recv()
        d_copy(0, 1 + way, core).start()
    lax.fori_loop(1, n_z, step, 0)
    near_ready(last)
    multiply(last, 0, FAR, (0, 1, 2), 0, units // 2)
    pass_far(last - 1)
    multiply(last, 0, FAR, (0, 1, 2), units // 2, units // 2)
    near_ready(last - 1)
    far_ready(last - 1)
    multiply(last - 1, 0, FAR + FAR_ROWS, (0, 1, 2, 3), 0, units // 2)
    pass_far(last)
    multiply(last - 1, 0, FAR + FAR_ROWS, (0, 1, 2, 3), units // 2, units // 2)
    far_ready(last)
    multiply(last, FAR, FAR_ROWS, (3,), 0, units)

    hidden_max = jnp.max(jnp.max(hidden_peak[...], axis=0, keepdims=True), axis=1, keepdims=True) / own_in
    hidden_row = jnp.where(iota((1, 128), 1) == z, hidden_max, 0.0)
    current = jnp.where(iota((2, 128), 0) == 0, peaks[...], hidden_row)
    base = 0
    for turn, phase in enumerate(peers):
        message[turn] = current
        for j, peer in enumerate(phase):
            remote(message.at[turn], inbox.at[base + j], m_send.at[base + j], m_recv.at[base + j], peer).start()
        for j, peer in enumerate(phase):
            remote(message.at[turn], inbox.at[base + j], m_send.at[base + j], m_recv.at[base + j], peer).wait_recv()
            current = jnp.maximum(current, inbox[base + j])
        base += len(phase)

    new_grad[...] = jnp.concatenate([hist_grad[...][1:], current[0:1, 0:n_z]], axis=0)
    new_hidden[...] = jnp.concatenate([hist_hidden[...][1:], current[1:2, 0:n_z]], axis=0)

    def drain(k, carry):
        @pl.when(k >= 1)
        def _():
            z_copy(k).wait_send()
            x_copy(k, 0).wait_send()
            x_copy(k, 1).wait_send()

        for way in range(2):
            f_copy(k, way).wait_send()
        for piece in range(5):
            d_copy(k, piece, core).wait_send()
        return carry

    for way in range(2):
        for late in range(2):
            first_copy(way, late).wait_send()
    lax.fori_loop(0, n_z, drain, 0)
    base = 0
    for turn, phase in enumerate(peers):
        for j, peer in enumerate(phase):
            remote(message.at[turn], inbox.at[base + j], m_send.at[base + j], m_recv.at[base + j], peer).wait_send()
        base += len(phase)


def write_out(*refs):
    count = len(refs) // 2
    sems = refs[-1]
    copies = []
    for i in range(3):
        cuts = PIECES if i == 0 else 1
        size = refs[i].shape[0] // cuts
        for j in range(cuts):
            source, target = (ref.at[pl.ds(j * size, size)] for ref in (refs[i], refs[count + i]))
            copies.append(pltpu.make_async_copy(source, target, sems.at[len(copies)]))
    for copy in copies:
        copy.start()
    for copy in copies:
        copy.wait()


def solution(mesh):
    n_y = mesh.shape["dp"]
    n_expert = mesh.shape["expert"]

    def per_device(grad_out, expert_ids, down_weight, history_grad, history_hidden):
        tok, features = grad_out.shape
        n_z = history_grad.shape[1]
        members = n_expert // n_z
        n_x = members // CORES
        units = down_weight.shape[1]
        capacity = tok * 9 // 32
        width = features * (capacity - MAIN) // MAIN
        n_messages = n_y * members - 1 + n_z - 1
        dma = pltpu.SemaphoreType.DMA
        anywhere = pl.BlockSpec(memory_space=pl.ANY)
        vmem, hbm = pl.BlockSpec(memory_space=pltpu.VMEM), pl.BlockSpec(memory_space=pltpu.HBM)
        small = jax.ShapeDtypeStruct(history_grad.shape, F32)
        arguments = expert_ids.T, history_grad, history_hidden, grad_out, down_weight[0]
        results = pl.pallas_call(
            functools.partial(kernel, n_y, n_z, n_x, capacity),
            out_shape=(jax.ShapeDtypeStruct((n_expert // CORES, CORES * capacity, units), BF16), small, small),
            in_specs=[hbm] * 5,
            out_specs=(vmem, vmem, vmem),
            scratch_shapes=[
                pltpu.VMEM((2, tok), jnp.int32),
                pltpu.VMEM(history_grad.shape, F32),
                pltpu.VMEM(history_grad.shape, F32),
                pltpu.VMEM((tok, features), BF16),
                pltpu.VMEM((units, features), BF16),
                pltpu.VMEM((n_z, MAIN, features + width), BF16),
                pltpu.VMEM((n_z, FAR + FAR_ROWS, features + width), BF16),
                pltpu.VMEM((n_z, tok), F32),
                pltpu.VMEM((NEAR, NEAR), BF16),
                pltpu.VMEM((PAIR, PAIR), BF16),
                pltpu.VMEM((1, 128), F32),
                pltpu.VMEM((8, 128), F32),
                pltpu.VMEM((2, 2, 128), F32),
                pltpu.VMEM((n_messages, 2, 128), F32),
                dma((5,)),
                dma((n_z,)), dma((n_z,)),
                dma((2, 2)), dma((2, 2)),
                dma((n_z, 2)), dma((n_z, 2)),
                dma((n_z, 2)), dma((n_z, 2)),
                dma((n_z, 5)), dma((n_z, 5)),
                dma((n_messages,)), dma((n_messages,)),
            ],
            compiler_params=pltpu.CompilerParams(
                collective_id=0, has_side_effects=True, vmem_limit_bytes=46 * 1024 * 1024
            ),
        )(*(pltpu.with_memory_space_constraint(a, pltpu.HBM) for a in arguments))
        rows, new_grad, new_hidden = pl.pallas_call(
            write_out,
            out_shape=tuple(jax.ShapeDtypeStruct(a.shape, a.dtype) for a in results),
            in_specs=[anywhere] * 3,
            out_specs=(hbm,) * 3,
            scratch_shapes=[dma((PIECES + 2,))],
            compiler_params=pltpu.CompilerParams(vmem_limit_bytes=1024 * 1024),
        )(*results)
        return rows.reshape(1, 1, n_expert * capacity, units), new_grad, new_hidden

    both = ("dp", "expert")
    return jax.shard_map(
        per_device,
        mesh=mesh,
        in_specs=(P(both, None), P(both, None), P("expert", None, None), P(), P()),
        out_specs=(P("dp", "expert", None, None), P(), P()),
        check_vma=False,
    )
```

```python
import functools

import jax
import jax.numpy as jnp
from jax import lax
from jax.experimental import pallas as pl
from jax.experimental.pallas import tpu as pltpu
from jax.sharding import PartitionSpec as P

MESH = pl.DeviceIdType.MESH
F32, BF16 = jnp.float32, jnp.bfloat16
CORES = 2
MAIN = 32
HALF = MAIN // 2
PAIR = CORES * MAIN
NEAR = 3 * PAIR
FAR = NEAR + 32
FAR_ROWS = PAIR + 16
TURNED = 256
EARLY = 5
PIECES = 8


def iota(shape, axis):
    return lax.broadcasted_iota(jnp.int32, shape, axis)


def unfold_matrix(rows, tail, fold):
    extra = rows // MAIN * tail
    goes, comes = iota((rows, rows), 0), iota((rows, rows), 1)
    part = functools.reduce(lambda a, b: a + b, [(goes >= extra * i).astype(jnp.int32) for i in range(1, fold)])
    rest = goes - part * extra
    wanted = rest // tail * MAIN + part * tail + rest % tail
    return (wanted == comes).astype(F32).astype(BF16)


def kernel(
    n_y, n_z, n_x, capacity,
    ids_hbm, hist_grad_hbm, hist_hidden_hbm, grad_hbm, weight_hbm,
    out_ref, new_grad, new_hidden,
    ids_ref, hist_grad, hist_hidden, grad_v, weight_v, weight_t, queue, gathered, slot_of, unfold_near, unfold_far, peaks, hidden_peak, message, inbox,
    local_sem, z_send, z_recv, o_send, o_recv, x_send, x_recv, f_send, f_recv, d_send, d_recv, m_send, m_recv, h_send,
):
    tok, features = grad_v.shape
    units = weight_v.shape[0]
    tail = capacity - MAIN
    fold = MAIN // tail
    width = features // fold
    members = n_x * CORES

    y = lax.axis_index("dp")
    me = lax.axis_index("expert")
    core = me % CORES
    x = (me // CORES) % n_x
    z = me // members
    group = me % members

    def at(to_z, to_x, to_core):
        return (y, (to_z * n_x + to_x) * CORES + to_core)

    right, left, far = (x + 1) % n_x, (x + n_x - 1) % n_x, (x + 2) % n_x
    partner = at(z, x, 1 - core)
    sides = (at(z, right, core), at(z, left, core))

    peers = [
        [
            ((y + i) % n_y, z * members + (group + j) % members)
            for i in range(n_y) for j in range(members) if i + j > 0
        ],
        [at((z + j) % n_z, x, 1 - core) for j in range(1, n_z)],
        [at((z + j) % n_z, x, core) for j in range(1, n_z)],
    ]
    barrier = pltpu.get_barrier_semaphore()
    for phase in peers[::-1]:
        for peer in phase:
            pl.semaphore_signal(barrier, inc=1, device_id=peer, device_id_type=MESH)

    pairs = (ids_hbm, ids_ref), (hist_grad_hbm, hist_grad), (hist_hidden_hbm, hist_hidden), (grad_hbm, grad_v), (weight_hbm, weight_v)
    loads = [pltpu.make_async_copy(source, target, local_sem.at[i]) for i, (source, target) in enumerate(pairs)]
    for load in loads:
        load.start()
    grad_in, weight_in = loads[3:]
    for load in loads[:3]:
        load.wait()

    ids = ids_ref[...]
    named = (iota((n_z, tok), 0) == ids[0:1, :]) | (iota((n_z, tok), 0) == ids[1:2, :])
    earlier = (iota((tok, tok), 0) < iota((tok, tok), 1)).astype(F32).astype(BF16)
    before = jnp.dot(named.astype(F32).astype(BF16), earlier, preferred_element_type=F32)
    slot_of[...] = jnp.where(named, before, -1.0)

    scale_in = 1.0 / jnp.max(hist_grad[...], axis=0, keepdims=True)
    scale_hidden = 1.0 / jnp.max(hist_hidden[...], axis=0, keepdims=True)
    own = iota((1, n_z), 1) == z
    own_in = jnp.sum(jnp.where(own, scale_in, 0.0), axis=1, keepdims=True)
    own_hidden = jnp.sum(jnp.where(own, scale_hidden, 0.0), axis=1, keepdims=True)
    factor = own_hidden / own_in

    all_rows = n_z * MAIN
    slots = jnp.broadcast_to(slot_of[...][:, None, :], (n_z, MAIN, tok)).reshape(all_rows, tok)
    in_block = iota((all_rows, tok), 0) % MAIN
    pick_main = (slots == in_block.astype(F32)).astype(F32).astype(BF16)
    is_tail = slots == (in_block % tail + MAIN).astype(F32)
    row_scale = jnp.sum(
        jnp.where(iota((all_rows, n_z), 1) == iota((all_rows, n_z), 0) // MAIN, scale_in, 0.0), axis=1, keepdims=True
    )

    def scaled(values):
        return jnp.clip(values * row_scale, -1.0, 1.0).astype(BF16).reshape(n_z, MAIN, width)

    def folded_peak(values):
        return functools.reduce(jnp.maximum, [jnp.abs(values[:, i:i + 128]) for i in range(0, width, 128)])

    grad_in.wait()
    tails = jnp.zeros((all_rows, width), F32)
    peak = jnp.zeros((all_rows, 128), F32)
    for part in range(fold):
        piece = grad_v[:, part * width:(part + 1) * width]
        values = jnp.dot(pick_main, piece, preferred_element_type=F32)
        queue[:, :, part * width:(part + 1) * width] = scaled(values)
        peak = jnp.maximum(peak, folded_peak(values))
        pick = (is_tail & (in_block // tail == part)).astype(F32).astype(BF16)
        tails = tails + jnp.dot(pick, piece, preferred_element_type=F32)
    queue[:, :, features:] = scaled(tails)
    peak = jnp.maximum(peak, folded_peak(tails))
    peak = jnp.max(jnp.max(peak.reshape(n_z, MAIN, 128), axis=1), axis=1, keepdims=True)
    diagonal = jnp.where(iota((n_z, 128), 0) == iota((n_z, 128), 1), peak, 0.0)
    peaks[...] = jnp.max(diagonal, axis=0, keepdims=True)
    hidden_peak[...] = jnp.zeros_like(hidden_peak)
    gathered[0, pl.ds(pl.multiple_of(core * MAIN, MAIN), MAIN), :] = queue[z]
    unfold_near[...] = unfold_matrix(NEAR, tail, fold)
    unfold_far[...] = unfold_matrix(PAIR, tail, fold)

    pl.semaphore_wait(barrier, sum(len(phase) for phase in peers))

    starts = (0, PAIR, 2 * PAIR, FAR)

    def offset(k):
        return ((k + 1) // 2) * (2 * (k % 2) - 1)

    def part_of(k, place, whose, low=0, count=MAIN):
        start = pl.multiple_of(starts[place] + whose * MAIN + low, HALF)
        return gathered.at[k, pl.ds(start, count), :]

    def remote(source, target, send, recv, device):
        return pltpu.make_async_remote_copy(
            src_ref=source, dst_ref=target, send_sem=send, recv_sem=recv, device_id=device, device_id_type=MESH
        )

    def z_copy(k):
        to_z = (z - offset(k) + n_z) % n_z
        return remote(queue.at[to_z], part_of(k, 0, core), z_send.at[k], z_recv.at[k], at(to_z, x, core))

    def x_copy(k, way):
        return remote(
            part_of(k, 0, core), part_of(k, 1 + way, core), x_send.at[k, way], x_recv.at[k, way], sides[way]
        )

    def first_copy(way, late):
        low = HALF * (way ^ late)
        return remote(
            part_of(0, 0, core, low, HALF), part_of(0, 1 + way, core, low, HALF),
            o_send.at[way, late], o_recv.at[way, late], sides[way],
        )

    def f_copy(k, way):
        return remote(
            part_of(k, 1 + way, core, way * HALF, HALF), part_of(k, 3, core, way * HALF, HALF),
            f_send.at[k, way], f_recv.at[k, way], sides[way],
        )

    def d_copy(k, piece, whose):
        if piece < 3:
            block = part_of(k, piece, whose)
        else:
            block = part_of(k, 3, whose, (piece - 3) * HALF, HALF)
        return remote(block, block, d_send.at[k, piece], d_recv.at[k, piece], partner)

    def pass_far(k):
        for way in range(2):
            f_copy(k, way).wait_recv()
            d_copy(k, 3 + way, core).start()

    def place_tails(k, low, rows, unfold):
        extra = rows // MAIN * tail
        room = -(-extra // 16) * 16
        folded = gathered[k, low:low + rows, features:features + width]
        plain = jnp.dot(unfold[...], folded, preferred_element_type=F32)
        for part in range(fold):
            piece = plain[part * extra:(part + 1) * extra]
            piece = jnp.concatenate([piece, jnp.zeros((room - extra, width), F32)], axis=0).astype(BF16)
            gathered[k, low + rows:low + rows + room, part * width:(part + 1) * width] = piece

    def multiply(k, low, rows, places, first, count):
        product = lax.dot_general(
            gathered[k, low:low + rows, 0:features], weight_t[:, first:first + count],
            (((1,), (0,)), ((), ())), preferred_element_type=F32,
        )
        size = jnp.max(jnp.abs(product).reshape(rows // 8, 8, count), axis=0)
        size = functools.reduce(jnp.maximum, [size[:, i:i + 128] for i in range(0, count, 128)])
        hidden_peak[...] = jnp.maximum(hidden_peak[...], size)
        result = jnp.clip(product * factor, -1.0, 1.0)
        from_z = (z + offset(k) + n_z) % n_z
        for place in places:
            start = starts[place] - low
            last = (NEAR + place * CORES * tail if place < 3 else FAR + PAIR) - low
            pieces = []
            for member in range(CORES):
                pieces.append(result[start + member * MAIN:start + (member + 1) * MAIN])
                pieces.append(result[last + member * tail:last + (member + 1) * tail])
            ordered = jnp.concatenate(pieces, axis=0).astype(BF16)
            out_ref[from_z * n_x + (x, left, right, far)[place], :, first:first + count] = ordered

    def near_ready(k):
        for piece in range(3):
            d_copy(k, piece, 1 - core).wait_recv()
        place_tails(k, 0, NEAR, unfold_near)

    def far_ready(k):
        for piece in range(3, 5):
            d_copy(k, piece, 1 - core).wait_recv()
        place_tails(k, FAR, PAIR, unfold_far)

    def send_own(k):
        x_copy(k, 0).start()
        x_copy(k, 1).start()
        d_copy(k, 0, core).start()

    def z_body(k, carry):
        z_copy(k).start()
        return carry

    for late in range(2):
        for way in range(2):
            first_copy(way, late).start()
    lax.fori_loop(1, n_z, z_body, 0)
    d_copy(0, 0, core).start()
    weight_in.wait()

    last = n_z - 1

    def transpose(block, carry):
        start = pl.multiple_of(block * TURNED, TURNED)
        weight_t[pl.ds(start, TURNED), :] = weight_v[:, pl.ds(start, TURNED)].T
        return carry

    blocks = features // TURNED
    early = blocks * EARLY // 12

    def step(i, carry):
        @pl.when(i < last)
        def _():
            z_copy(i + 1).wait_recv()
            send_own(i + 1)

        @pl.when(i == 1)
        def _():
            lax.fori_loop(early, blocks, transpose, 0)

        @pl.when(i >= 2)
        def _():
            k = i - 2
            pass_far(k)
            near_ready(k)
            far_ready(k)
            multiply(k, 0, FAR + FAR_ROWS, (0, 1, 2, 3), 0, units)

        for way in range(2):
            x_copy(i, way).wait_recv()
            f_copy(i, way).start()
            d_copy(i, 1 + way, core).start()
        return carry

    lax.fori_loop(0, early, transpose, 0)
    for way in range(2):
        first_copy(way, 0).wait_recv()
        f_copy(0, way).start()
    z_copy(1).wait_recv()
    send_own(1)
    for way in range(2):
        first_copy(way, 1).wait_recv()
        d_copy(0, 1 + way, core).start()
    lax.fori_loop(1, n_z, step, 0)
    near_ready(last)
    multiply(last, 0, FAR, (0, 1, 2), 0, units // 2)
    pass_far(last - 1)
    multiply(last, 0, FAR, (0, 1, 2), units // 2, units // 2)
    near_ready(last - 1)
    far_ready(last - 1)
    multiply(last - 1, 0, FAR + FAR_ROWS, (0, 1, 2, 3), 0, units // 2)
    pass_far(last)
    multiply(last - 1, 0, FAR + FAR_ROWS, (0, 1, 2, 3), units // 2, units // 2)
    far_ready(last)
    multiply(last, FAR, FAR_ROWS, (3,), 0, units)

    hidden_max = jnp.max(jnp.max(hidden_peak[...], axis=0, keepdims=True), axis=1, keepdims=True) / own_in
    hidden_row = jnp.where(iota((1, 128), 1) == z, hidden_max, 0.0)
    current = jnp.where(iota((2, 128), 0) == 0, peaks[...], hidden_row)
    def m_copy(turn, slot, peer):
        return remote(message.at[turn], inbox.at[slot], m_send.at[slot], m_recv.at[slot], peer)

    def to_hubs(act):
        for slot, peer in enumerate(peers[0]):
            pl.when((core + slot + 1) % CORES == 1)(functools.partial(act, m_copy(0, slot, peer)))

    def hub_copy(place, slot, peer):
        slot = len(peers[0]) + slot
        return remote(message.at[1], inbox.at[slot], h_send.at[place], m_recv.at[slot], peer)

    hub_copies = [hub_copy(to * (n_z - 1) + j, j, peers[1 + to][j]) for to in range(2) for j in range(n_z - 1)]
    hub_copies.append(hub_copy(2 * (n_z - 1), n_z - 1, partner))
    message[0] = current
    to_hubs(lambda copy: copy.start())

    @pl.when(core == 1)
    def _():
        total = message[0]
        for slot, peer in enumerate(peers[0]):
            m_copy(0, slot, peer).wait_recv()
            total = jnp.maximum(total, inbox[slot])
        message[1] = total
        for copy in hub_copies:
            copy.start()

    @pl.when(core == 0)
    def _():
        hub_copies[-1].wait_recv()
        message[1] = inbox[len(peers[0]) + n_z - 1]

    current = message[1]
    for j in range(n_z - 1):
        hub_copies[j].wait_recv()
        current = jnp.maximum(current, inbox[len(peers[0]) + j])

    new_grad[...] = jnp.concatenate([hist_grad[...][1:], current[0:1, 0:n_z]], axis=0)
    new_hidden[...] = jnp.concatenate([hist_hidden[...][1:], current[1:2, 0:n_z]], axis=0)

    def drain(k, carry):
        @pl.when(k >= 1)
        def _():
            z_copy(k).wait_send()
            x_copy(k, 0).wait_send()
            x_copy(k, 1).wait_send()

        for way in range(2):
            f_copy(k, way).wait_send()
        for piece in range(5):
            d_copy(k, piece, core).wait_send()
        return carry

    for way in range(2):
        for late in range(2):
            first_copy(way, late).wait_send()
    lax.fori_loop(0, n_z, drain, 0)
    to_hubs(lambda copy: copy.wait_send())

    @pl.when(core == 1)
    def _():
        for copy in hub_copies:
            copy.wait_send()


def write_out(*refs):
    count = len(refs) // 2
    sems = refs[-1]
    copies = []
    for i in range(3):
        cuts = PIECES if i == 0 else 1
        size = refs[i].shape[0] // cuts
        for j in range(cuts):
            source, target = (ref.at[pl.ds(j * size, size)] for ref in (refs[i], refs[count + i]))
            copies.append(pltpu.make_async_copy(source, target, sems.at[len(copies)]))
    for copy in copies:
        copy.start()
    for copy in copies:
        copy.wait()


def solution(mesh):
    n_y = mesh.shape["dp"]
    n_expert = mesh.shape["expert"]

    def per_device(grad_out, expert_ids, down_weight, history_grad, history_hidden):
        tok, features = grad_out.shape
        n_z = history_grad.shape[1]
        members = n_expert // n_z
        n_x = members // CORES
        units = down_weight.shape[1]
        capacity = tok * 9 // 32
        width = features * (capacity - MAIN) // MAIN
        n_messages = n_y * members - 1 + n_z
        dma = pltpu.SemaphoreType.DMA
        anywhere = pl.BlockSpec(memory_space=pl.ANY)
        vmem, hbm = pl.BlockSpec(memory_space=pltpu.VMEM), pl.BlockSpec(memory_space=pltpu.HBM)
        small = jax.ShapeDtypeStruct(history_grad.shape, F32)
        arguments = expert_ids.T, history_grad, history_hidden, grad_out, down_weight[0]
        results = pl.pallas_call(
            functools.partial(kernel, n_y, n_z, n_x, capacity),
            out_shape=(jax.ShapeDtypeStruct((n_expert // CORES, CORES * capacity, units), BF16), small, small),
            in_specs=[hbm] * 5,
            out_specs=(vmem, vmem, vmem),
            scratch_shapes=[
                pltpu.VMEM((2, tok), jnp.int32),
                pltpu.VMEM(history_grad.shape, F32),
                pltpu.VMEM(history_grad.shape, F32),
                pltpu.VMEM((tok, features), BF16),
                pltpu.VMEM((units, features), BF16),
                pltpu.VMEM((features, units), BF16),
                pltpu.VMEM((n_z, MAIN, features + width), BF16),
                pltpu.VMEM((n_z, FAR + FAR_ROWS, features + width), BF16),
                pltpu.VMEM((n_z, tok), F32),
                pltpu.VMEM((NEAR, NEAR), BF16),
                pltpu.VMEM((PAIR, PAIR), BF16),
                pltpu.VMEM((1, 128), F32),
                pltpu.VMEM((8, 128), F32),
                pltpu.VMEM((2, 2, 128), F32),
                pltpu.VMEM((n_messages, 2, 128), F32),
                dma((5,)),
                dma((n_z,)), dma((n_z,)),
                dma((2, 2)), dma((2, 2)),
                dma((n_z, 2)), dma((n_z, 2)),
                dma((n_z, 2)), dma((n_z, 2)),
                dma((n_z, 5)), dma((n_z, 5)),
                dma((n_messages,)), dma((n_messages,)), dma((2 * n_z - 1,)),
            ],
            compiler_params=pltpu.CompilerParams(
                collective_id=0, has_side_effects=True, vmem_limit_bytes=46 * 1024 * 1024
            ),
        )(*(pltpu.with_memory_space_constraint(a, pltpu.HBM) for a in arguments))
        rows, new_grad, new_hidden = pl.pallas_call(
            write_out,
            out_shape=tuple(jax.ShapeDtypeStruct(a.shape, a.dtype) for a in results),
            in_specs=[anywhere] * 3,
            out_specs=(hbm,) * 3,
            scratch_shapes=[dma((PIECES + 2,))],
            compiler_params=pltpu.CompilerParams(vmem_limit_bytes=1024 * 1024),
        )(*results)
        return rows.reshape(1, 1, n_expert * capacity, units), new_grad, new_hidden

    both = ("dp", "expert")
    return jax.shard_map(
        per_device,
        mesh=mesh,
        in_specs=(P(both, None), P(both, None), P("expert", None, None), P(), P()),
        out_specs=(P("dp", "expert", None, None), P(), P()),
        check_vma=False,
    )
```

```python
import functools

import jax
import jax.numpy as jnp
from jax import lax
from jax.experimental import pallas as pl
from jax.experimental.pallas import tpu as pltpu
from jax.sharding import PartitionSpec as P

MESH = pl.DeviceIdType.MESH
F32, BF16 = jnp.float32, jnp.bfloat16
CORES = 2
MAIN = 32
HALF = MAIN // 2
PAIR = CORES * MAIN
NEAR = 3 * PAIR
FAR = NEAR + 32
FAR_ROWS = PAIR + 16
TURNED = 256
EARLY = 5
PIECES = 8


def iota(shape, axis):
    return lax.broadcasted_iota(jnp.int32, shape, axis)


def unfold_matrix(rows, tail, fold):
    extra = rows // MAIN * tail
    goes, comes = iota((rows, rows), 0), iota((rows, rows), 1)
    part = functools.reduce(lambda a, b: a + b, [(goes >= extra * i).astype(jnp.int32) for i in range(1, fold)])
    rest = goes - part * extra
    wanted = rest // tail * MAIN + part * tail + rest % tail
    return (wanted == comes).astype(F32).astype(BF16)


def kernel(
    n_y, n_z, n_x, capacity,
    ids_hbm, hist_grad_hbm, hist_hidden_hbm, grad_hbm, weight_hbm,
    out_ref, new_grad, new_hidden,
    ids_ref, hist_grad, hist_hidden, grad_v, weight_v, weight_t, queue, gathered, slot_of, unfold_near, unfold_far, peaks, hidden_peak, message, inbox,
    local_sem, z_send, z_recv, o_send, o_recv, x_send, x_recv, f_send, f_recv, d_send, d_recv, m_send, m_recv, h_send,
):
    tok, features = grad_v.shape
    units = weight_v.shape[0]
    tail = capacity - MAIN
    fold = MAIN // tail
    width = features // fold
    members = n_x * CORES

    y = lax.axis_index("dp")
    me = lax.axis_index("expert")
    core = me % CORES
    x = (me // CORES) % n_x
    z = me // members
    group = me % members

    def at(to_z, to_x, to_core):
        return (y, (to_z * n_x + to_x) * CORES + to_core)

    right, left, far = (x + 1) % n_x, (x + n_x - 1) % n_x, (x + 2) % n_x
    partner = at(z, x, 1 - core)
    sides = (at(z, right, core), at(z, left, core))

    peers = [
        [
            ((y + i) % n_y, z * members + (group + j) % members)
            for i in range(n_y) for j in range(members) if i + j > 0
        ],
        [at((z + j) % n_z, x, 1 - core) for j in range(1, n_z)],
        [at((z + j) % n_z, x, core) for j in range(1, n_z)],
    ]
    barrier = pltpu.get_barrier_semaphore()
    for phase in peers[::-1]:
        for peer in phase:
            pl.semaphore_signal(barrier, inc=1, device_id=peer, device_id_type=MESH)

    pairs = (ids_hbm, ids_ref), (hist_grad_hbm, hist_grad), (hist_hidden_hbm, hist_hidden), (grad_hbm, grad_v), (weight_hbm, weight_v)
    loads = [pltpu.make_async_copy(source, target, local_sem.at[i]) for i, (source, target) in enumerate(pairs)]
    for load in loads:
        load.start()
    grad_in, weight_in = loads[3:]
    for load in loads[:3]:
        load.wait()

    ids = ids_ref[...]
    named = (iota((n_z, tok), 0) == ids[0:1, :]) | (iota((n_z, tok), 0) == ids[1:2, :])
    earlier = (iota((tok, tok), 0) < iota((tok, tok), 1)).astype(F32).astype(BF16)
    before = jnp.dot(named.astype(F32).astype(BF16), earlier, preferred_element_type=F32)
    slot_of[...] = jnp.where(named, before, -1.0)

    scale_in = 1.0 / jnp.max(hist_grad[...], axis=0, keepdims=True)
    scale_hidden = 1.0 / jnp.max(hist_hidden[...], axis=0, keepdims=True)
    own = iota((1, n_z), 1) == z
    own_in = jnp.sum(jnp.where(own, scale_in, 0.0), axis=1, keepdims=True)
    own_hidden = jnp.sum(jnp.where(own, scale_hidden, 0.0), axis=1, keepdims=True)
    factor = own_hidden / own_in

    all_rows = n_z * MAIN
    slots = jnp.broadcast_to(slot_of[...][:, None, :], (n_z, MAIN, tok)).reshape(all_rows, tok)
    in_block = iota((all_rows, tok), 0) % MAIN
    pick_main = (slots == in_block.astype(F32)).astype(F32).astype(BF16)
    is_tail = slots == (in_block % tail + MAIN).astype(F32)
    row_scale = jnp.sum(
        jnp.where(iota((all_rows, n_z), 1) == iota((all_rows, n_z), 0) // MAIN, scale_in, 0.0), axis=1, keepdims=True
    )

    def scaled(values):
        return jnp.clip(values * row_scale, -1.0, 1.0).astype(BF16).reshape(n_z, MAIN, width)

    def folded_peak(values):
        return functools.reduce(jnp.maximum, [jnp.abs(values[:, i:i + 128]) for i in range(0, width, 128)])

    grad_in.wait()
    tails = jnp.zeros((all_rows, width), F32)
    peak = jnp.zeros((all_rows, 128), F32)
    for part in range(fold):
        piece = grad_v[:, part * width:(part + 1) * width]
        values = jnp.dot(pick_main, piece, preferred_element_type=F32)
        queue[:, :, part * width:(part + 1) * width] = scaled(values)
        peak = jnp.maximum(peak, folded_peak(values))
        pick = (is_tail & (in_block // tail == part)).astype(F32).astype(BF16)
        tails = tails + jnp.dot(pick, piece, preferred_element_type=F32)
    queue[:, :, features:] = scaled(tails)
    peak = jnp.maximum(peak, folded_peak(tails))
    peak = jnp.max(jnp.max(peak.reshape(n_z, MAIN, 128), axis=1), axis=1, keepdims=True)
    diagonal = jnp.where(iota((n_z, 128), 0) == iota((n_z, 128), 1), peak, 0.0)
    peaks[...] = jnp.max(diagonal, axis=0, keepdims=True)
    hidden_peak[...] = jnp.zeros_like(hidden_peak)
    gathered[0, pl.ds(pl.multiple_of(core * MAIN, MAIN), MAIN), :] = queue[z]
    unfold_near[...] = unfold_matrix(NEAR, tail, fold)
    unfold_far[...] = unfold_matrix(PAIR, tail, fold)

    pl.semaphore_wait(barrier, sum(len(phase) for phase in peers))

    starts = (0, PAIR, 2 * PAIR, FAR)

    def offset(k):
        return ((k + 1) // 2) * (2 * (k % 2) - 1)

    def part_of(k, place, whose, low=0, count=MAIN):
        start = pl.multiple_of(starts[place] + whose * MAIN + low, HALF)
        return gathered.at[k, pl.ds(start, count), :]

    def remote(source, target, send, recv, device):
        return pltpu.make_async_remote_copy(
            src_ref=source, dst_ref=target, send_sem=send, recv_sem=recv, device_id=device, device_id_type=MESH
        )

    def z_copy(k):
        to_z = (z - offset(k) + n_z) % n_z
        return remote(queue.at[to_z], part_of(k, 0, core), z_send.at[k], z_recv.at[k], at(to_z, x, core))

    def x_copy(k, way):
        return remote(
            part_of(k, 0, core), part_of(k, 1 + way, core), x_send.at[k, way], x_recv.at[k, way], sides[way]
        )

    def first_copy(way, late):
        low = HALF * (way ^ late)
        return remote(
            part_of(0, 0, core, low, HALF), part_of(0, 1 + way, core, low, HALF),
            o_send.at[way, late], o_recv.at[way, late], sides[way],
        )

    def f_copy(k, way):
        return remote(
            part_of(k, 1 + way, core, way * HALF, HALF), part_of(k, 3, core, way * HALF, HALF),
            f_send.at[k, way], f_recv.at[k, way], sides[way],
        )

    def d_copy(k, piece, whose):
        if piece < 3:
            block = part_of(k, piece, whose)
        else:
            block = part_of(k, 3, whose, (piece - 3) * HALF, HALF)
        return remote(block, block, d_send.at[k, piece], d_recv.at[k, piece], partner)

    def pass_far(k):
        for way in range(2):
            f_copy(k, way).wait_recv()
            d_copy(k, 3 + way, core).start()

    def place_tails(k, low, rows, unfold):
        extra = rows // MAIN * tail
        room = -(-extra // 16) * 16
        folded = gathered[k, low:low + rows, features:features + width]
        plain = jnp.dot(unfold[...], folded, preferred_element_type=F32)
        for part in range(fold):
            piece = plain[part * extra:(part + 1) * extra]
            piece = jnp.concatenate([piece, jnp.zeros((room - extra, width), F32)], axis=0).astype(BF16)
            gathered[k, low + rows:low + rows + room, part * width:(part + 1) * width] = piece

    def multiply(k, low, rows, places, first, count):
        product = lax.dot_general(
            gathered[k, low:low + rows, 0:features], weight_t[:, first:first + count],
            (((1,), (0,)), ((), ())), preferred_element_type=F32,
        )
        size = jnp.max(jnp.abs(product).reshape(rows // 8, 8, count), axis=0)
        size = functools.reduce(jnp.maximum, [size[:, i:i + 128] for i in range(0, count, 128)])
        hidden_peak[...] = jnp.maximum(hidden_peak[...], size)
        result = jnp.clip(product * factor, -1.0, 1.0)
        from_z = (z + offset(k) + n_z) % n_z
        for place in places:
            start = starts[place] - low
            last = (NEAR + place * CORES * tail if place < 3 else FAR + PAIR) - low
            pieces = []
            for member in range(CORES):
                pieces.append(result[start + member * MAIN:start + (member + 1) * MAIN])
                pieces.append(result[last + member * tail:last + (member + 1) * tail])
            ordered = jnp.concatenate(pieces, axis=0).astype(BF16)
            out_ref[from_z * n_x + (x, left, right, far)[place], :, first:first + count] = ordered

    def near_ready(k):
        for piece in range(3):
            d_copy(k, piece, 1 - core).wait_recv()
        place_tails(k, 0, NEAR, unfold_near)

    def far_ready(k):
        for piece in range(3, 5):
            d_copy(k, piece, 1 - core).wait_recv()
        place_tails(k, FAR, PAIR, unfold_far)

    def send_own(k):
        x_copy(k, 0).start()
        x_copy(k, 1).start()
        d_copy(k, 0, core).start()

    def z_body(k, carry):
        z_copy(k).start()
        return carry

    for late in range(2):
        for way in range(2):
            first_copy(way, late).start()
    lax.fori_loop(1, n_z, z_body, 0)
    d_copy(0, 0, core).start()
    weight_in.wait()

    last = n_z - 1

    def transpose(block, carry):
        start = pl.multiple_of(block * TURNED, TURNED)
        weight_t[pl.ds(start, TURNED), :] = weight_v[:, pl.ds(start, TURNED)].T
        return carry

    blocks = features // TURNED
    early = blocks * EARLY // 12

    def step(i, carry):
        @pl.when(i < last)
        def _():
            z_copy(i + 1).wait_recv()
            send_own(i + 1)

        @pl.when(i == 1)
        def _():
            lax.fori_loop(early, blocks, transpose, 0)

        @pl.when(i >= 2)
        def _():
            k = i - 2
            pass_far(k)
            near_ready(k)
            far_ready(k)
            multiply(k, 0, FAR + FAR_ROWS, (0, 1, 2, 3), 0, units)

        for way in range(2):
            x_copy(i, way).wait_recv()
            f_copy(i, way).start()
            d_copy(i, 1 + way, core).start()
        return carry

    lax.fori_loop(0, early, transpose, 0)
    for way in range(2):
        first_copy(way, 0).wait_recv()
        f_copy(0, way).start()
    z_copy(1).wait_recv()
    send_own(1)
    for way in range(2):
        first_copy(way, 1).wait_recv()
        d_copy(0, 1 + way, core).start()
    lax.fori_loop(1, n_z, step, 0)
    near_ready(last)
    multiply(last, 0, FAR, (0, 1, 2), 0, units // 2)
    pass_far(last - 1)
    multiply(last, 0, FAR, (0, 1, 2), units // 2, units // 2)
    near_ready(last - 1)
    far_ready(last - 1)
    multiply(last - 1, 0, FAR + FAR_ROWS, (0, 1, 2, 3), 0, units // 2)
    pass_far(last)
    multiply(last - 1, 0, FAR + FAR_ROWS, (0, 1, 2, 3), units // 2, units // 2)
    far_ready(last)
    multiply(last, FAR, FAR_ROWS, (3,), 0, units)

    hidden_max = jnp.max(jnp.max(hidden_peak[...], axis=0, keepdims=True), axis=1, keepdims=True) / own_in
    hidden_row = jnp.where(iota((1, 128), 1) == z, hidden_max, 0.0)
    current = jnp.where(iota((2, 128), 0) == 0, peaks[...], hidden_row)
    others = n_y * members - 1
    chips = [(i, j) for i in range(n_y) for j in range(n_x)]

    def gather_copy(index):
        i, j = chips[index]
        hub = ((y + i) % n_y, (z * n_x + (x + j) % n_x) * CORES + 1)
        slot = others - (index * CORES + 1 - core)
        return remote(message.at[0], inbox.at[slot], m_send.at[index], m_recv.at[0], hub)

    def hub_copy(place, slot, peer, sem):
        return remote(message.at[1], inbox.at[others + 1 + slot], h_send.at[place], m_recv.at[sem], peer)

    def arrived(low, count, sem):
        block = inbox.at[pl.ds(low, count)]
        remote(block, block, m_send.at[0], m_recv.at[sem], partner).wait_recv()
        return jnp.max(inbox[low:low + count], axis=0)

    hub_copies = [hub_copy(to * (n_z - 1) + j, j, peers[1 + to][j], 1) for to in range(2) for j in range(n_z - 1)]
    hub_copies.append(hub_copy(2 * (n_z - 1), n_z - 1, partner, 2))
    message[0] = current
    for index in range(1, len(chips)):
        gather_copy(index).start()

    @pl.when(core == 0)
    def _():
        gather_copy(0).start()
        message[1] = arrived(others + n_z, 1, 2)

    @pl.when(core == 1)
    def _():
        message[1] = jnp.maximum(message[0], arrived(0, others, 0))
        for copy in hub_copies:
            copy.start()

    current = jnp.maximum(message[1], arrived(others + 1, n_z - 1, 1))

    new_grad[...] = jnp.concatenate([hist_grad[...][1:], current[0:1, 0:n_z]], axis=0)
    new_hidden[...] = jnp.concatenate([hist_hidden[...][1:], current[1:2, 0:n_z]], axis=0)

    def drain(k, carry):
        @pl.when(k >= 1)
        def _():
            z_copy(k).wait_send()
            x_copy(k, 0).wait_send()
            x_copy(k, 1).wait_send()

        for way in range(2):
            f_copy(k, way).wait_send()
        for piece in range(5):
            d_copy(k, piece, core).wait_send()
        return carry

    for way in range(2):
        for late in range(2):
            first_copy(way, late).wait_send()
    lax.fori_loop(0, n_z, drain, 0)
    for index in range(1, len(chips)):
        gather_copy(index).wait_send()

    @pl.when(core == 0)
    def _():
        gather_copy(0).wait_send()

    @pl.when(core == 1)
    def _():
        for copy in hub_copies:
            copy.wait_send()


def write_out(*refs):
    count = len(refs) // 2
    sems = refs[-1]
    copies = []
    for i in range(3):
        cuts = PIECES if i == 0 else 1
        size = refs[i].shape[0] // cuts
        for j in range(cuts):
            source, target = (ref.at[pl.ds(j * size, size)] for ref in (refs[i], refs[count + i]))
            copies.append(pltpu.make_async_copy(source, target, sems.at[len(copies)]))
    for copy in copies:
        copy.start()
    for copy in copies:
        copy.wait()


def solution(mesh):
    n_y = mesh.shape["dp"]
    n_expert = mesh.shape["expert"]

    def per_device(grad_out, expert_ids, down_weight, history_grad, history_hidden):
        tok, features = grad_out.shape
        n_z = history_grad.shape[1]
        members = n_expert // n_z
        n_x = members // CORES
        units = down_weight.shape[1]
        capacity = tok * 9 // 32
        width = features * (capacity - MAIN) // MAIN
        n_messages = n_y * members + n_z
        dma = pltpu.SemaphoreType.DMA
        anywhere = pl.BlockSpec(memory_space=pl.ANY)
        vmem, hbm = pl.BlockSpec(memory_space=pltpu.VMEM), pl.BlockSpec(memory_space=pltpu.HBM)
        small = jax.ShapeDtypeStruct(history_grad.shape, F32)
        arguments = expert_ids.T, history_grad, history_hidden, grad_out, down_weight[0]
        results = pl.pallas_call(
            functools.partial(kernel, n_y, n_z, n_x, capacity),
            out_shape=(jax.ShapeDtypeStruct((n_expert // CORES, CORES * capacity, units), BF16), small, small),
            in_specs=[hbm] * 5,
            out_specs=(vmem, vmem, vmem),
            scratch_shapes=[
                pltpu.VMEM((2, tok), jnp.int32),
                pltpu.VMEM(history_grad.shape, F32),
                pltpu.VMEM(history_grad.shape, F32),
                pltpu.VMEM((tok, features), BF16),
                pltpu.VMEM((units, features), BF16),
                pltpu.VMEM((features, units), BF16),
                pltpu.VMEM((n_z, MAIN, features + width), BF16),
                pltpu.VMEM((n_z, FAR + FAR_ROWS, features + width), BF16),
                pltpu.VMEM((n_z, tok), F32),
                pltpu.VMEM((NEAR, NEAR), BF16),
                pltpu.VMEM((PAIR, PAIR), BF16),
                pltpu.VMEM((1, 128), F32),
                pltpu.VMEM((8, 128), F32),
                pltpu.VMEM((2, 2, 128), F32),
                pltpu.VMEM((n_messages, 2, 128), F32),
                dma((5,)),
                dma((n_z,)), dma((n_z,)),
                dma((2, 2)), dma((2, 2)),
                dma((n_z, 2)), dma((n_z, 2)),
                dma((n_z, 2)), dma((n_z, 2)),
                dma((n_z, 5)), dma((n_z, 5)),
                dma((n_y * n_x,)), dma((3,)), dma((2 * n_z - 1,)),
            ],
            compiler_params=pltpu.CompilerParams(
                collective_id=0, has_side_effects=True, vmem_limit_bytes=46 * 1024 * 1024
            ),
        )(*(pltpu.with_memory_space_constraint(a, pltpu.HBM) for a in arguments))
        rows, new_grad, new_hidden = pl.pallas_call(
            write_out,
            out_shape=tuple(jax.ShapeDtypeStruct(a.shape, a.dtype) for a in results),
            in_specs=[anywhere] * 3,
            out_specs=(hbm,) * 3,
            scratch_shapes=[dma((PIECES + 2,))],
            compiler_params=pltpu.CompilerParams(vmem_limit_bytes=1024 * 1024),
        )(*results)
        return rows.reshape(1, 1, n_expert * capacity, units), new_grad, new_hidden

    both = ("dp", "expert")
    return jax.shard_map(
        per_device,
        mesh=mesh,
        in_specs=(P(both, None), P(both, None), P("expert", None, None), P(), P()),
        out_specs=(P("dp", "expert", None, None), P(), P()),
        check_vma=False,
    )
```

```python
import functools

import jax
import jax.numpy as jnp
from jax import lax
from jax.experimental import pallas as pl
from jax.experimental.pallas import tpu as pltpu
from jax.sharding import PartitionSpec as P

MESH = pl.DeviceIdType.MESH
F32, BF16 = jnp.float32, jnp.bfloat16
CORES = 2
MAIN = 32
HALF = MAIN // 2
PAIR = CORES * MAIN
NEAR = 3 * PAIR
FAR = NEAR + 32
FAR_ROWS = PAIR + 16
TURNED = 256
EARLY = 5
PIECES = 8


def iota(shape, axis):
    return lax.broadcasted_iota(jnp.int32, shape, axis)


def unfold_matrix(rows, tail, fold):
    extra = rows // MAIN * tail
    goes, comes = iota((rows, rows), 0), iota((rows, rows), 1)
    part = functools.reduce(lambda a, b: a + b, [(goes >= extra * i).astype(jnp.int32) for i in range(1, fold)])
    rest = goes - part * extra
    wanted = rest // tail * MAIN + part * tail + rest % tail
    return (wanted == comes).astype(F32).astype(BF16)


def kernel(
    n_y, n_z, n_x, capacity,
    ids_hbm, hist_grad_hbm, hist_hidden_hbm, grad_hbm, weight_hbm,
    out_ref, new_grad, new_hidden,
    ids_ref, hist_grad, hist_hidden, grad_v, weight_v, weight_t, queue, gathered, slot_of, unfold_near, unfold_far, peaks, hidden_peak, message, inbox,
    local_sem, z_send, z_recv, o_send, o_recv, x_send, x_recv, f_send, f_recv, d_send, d_recv, m_send, m_recv, h_send,
):
    tok, features = grad_v.shape
    units = weight_v.shape[0]
    tail = capacity - MAIN
    fold = MAIN // tail
    width = features // fold
    members = n_x * CORES

    y = lax.axis_index("dp")
    me = lax.axis_index("expert")
    core = me % CORES
    x = (me // CORES) % n_x
    z = me // members
    group = me % members

    def at(to_z, to_x, to_core):
        return (y, (to_z * n_x + to_x) * CORES + to_core)

    right, left, far = (x + 1) % n_x, (x + n_x - 1) % n_x, (x + 2) % n_x
    partner = at(z, x, 1 - core)
    sides = (at(z, right, core), at(z, left, core))

    peers = [
        [
            ((y + i) % n_y, z * members + (group + j) % members)
            for i in range(n_y) for j in range(members) if i + j > 0
        ],
        [at((z + j) % n_z, x, 1 - core) for j in range(1, n_z)],
        [at((z + j) % n_z, x, core) for j in range(1, n_z)],
    ]
    barrier = pltpu.get_barrier_semaphore()
    for phase in peers[::-1]:
        for peer in phase:
            pl.semaphore_signal(barrier, inc=1, device_id=peer, device_id_type=MESH)

    pairs = (ids_hbm, ids_ref), (hist_grad_hbm, hist_grad), (hist_hidden_hbm, hist_hidden), (grad_hbm, grad_v), (weight_hbm, weight_v)
    loads = [pltpu.make_async_copy(source, target, local_sem.at[i]) for i, (source, target) in enumerate(pairs)]
    for load in loads:
        load.start()
    grad_in, weight_in = loads[3:]
    for load in loads[:3]:
        load.wait()

    ids = ids_ref[...]
    named = (iota((n_z, tok), 0) == ids[0:1, :]) | (iota((n_z, tok), 0) == ids[1:2, :])
    earlier = (iota((tok, tok), 0) < iota((tok, tok), 1)).astype(F32).astype(BF16)
    before = jnp.dot(named.astype(F32).astype(BF16), earlier, preferred_element_type=F32)
    slot_of[...] = jnp.where(named, before, -1.0)

    scale_in = 1.0 / jnp.max(hist_grad[...], axis=0, keepdims=True)
    scale_hidden = 1.0 / jnp.max(hist_hidden[...], axis=0, keepdims=True)
    own = iota((1, n_z), 1) == z
    own_in = jnp.sum(jnp.where(own, scale_in, 0.0), axis=1, keepdims=True)
    own_hidden = jnp.sum(jnp.where(own, scale_hidden, 0.0), axis=1, keepdims=True)
    factor = own_hidden / own_in

    all_rows = n_z * MAIN
    slots = jnp.broadcast_to(slot_of[...][:, None, :], (n_z, MAIN, tok)).reshape(all_rows, tok)
    in_block = iota((all_rows, tok), 0) % MAIN
    pick_main = (slots == in_block.astype(F32)).astype(F32).astype(BF16)
    is_tail = slots == (in_block % tail + MAIN).astype(F32)
    row_scale = jnp.sum(
        jnp.where(iota((all_rows, n_z), 1) == iota((all_rows, n_z), 0) // MAIN, scale_in, 0.0), axis=1, keepdims=True
    )

    def scaled(values):
        return jnp.clip(values * row_scale, -1.0, 1.0).astype(BF16).reshape(n_z, MAIN, width)

    def folded_peak(values):
        return functools.reduce(jnp.maximum, [jnp.abs(values[:, i:i + 128]) for i in range(0, width, 128)])

    grad_in.wait()
    tails = jnp.zeros((all_rows, width), F32)
    peak = jnp.zeros((all_rows, 128), F32)
    for part in range(fold):
        piece = grad_v[:, part * width:(part + 1) * width]
        values = jnp.dot(pick_main, piece, preferred_element_type=F32)
        queue[:, :, part * width:(part + 1) * width] = scaled(values)
        peak = jnp.maximum(peak, folded_peak(values))
        pick = (is_tail & (in_block // tail == part)).astype(F32).astype(BF16)
        tails = tails + jnp.dot(pick, piece, preferred_element_type=F32)
    queue[:, :, features:] = scaled(tails)
    peak = jnp.maximum(peak, folded_peak(tails))
    peak = jnp.max(jnp.max(peak.reshape(n_z, MAIN, 128), axis=1), axis=1, keepdims=True)
    diagonal = jnp.where(iota((n_z, 128), 0) == iota((n_z, 128), 1), peak, 0.0)
    peaks[...] = jnp.max(diagonal, axis=0, keepdims=True)
    hidden_peak[...] = jnp.zeros_like(hidden_peak)
    gathered[0, pl.ds(pl.multiple_of(core * MAIN, MAIN), MAIN), :] = queue[z]
    unfold_near[...] = unfold_matrix(NEAR, tail, fold)
    unfold_far[...] = unfold_matrix(PAIR, tail, fold)

    pl.semaphore_wait(barrier, sum(len(phase) for phase in peers))

    starts = (0, PAIR, 2 * PAIR, FAR)

    def offset(k):
        return ((k + 1) // 2) * (2 * (k % 2) - 1)

    def part_of(k, place, whose, low=0, count=MAIN):
        start = pl.multiple_of(starts[place] + whose * MAIN + low, HALF)
        return gathered.at[k, pl.ds(start, count), :]

    def remote(source, target, send, recv, device):
        return pltpu.make_async_remote_copy(
            src_ref=source, dst_ref=target, send_sem=send, recv_sem=recv, device_id=device, device_id_type=MESH
        )

    def z_copy(k):
        to_z = (z - offset(k) + n_z) % n_z
        return remote(queue.at[to_z], part_of(k, 0, core), z_send.at[k], z_recv.at[k], at(to_z, x, core))

    def x_copy(k, way):
        return remote(
            part_of(k, 0, core), part_of(k, 1 + way, core), x_send.at[k, way], x_recv.at[k, way], sides[way]
        )

    def z_half(late):
        to_z = (z - offset(1) + n_z) % n_z
        return remote(
            queue.at[to_z, pl.ds(late * HALF, HALF), :], part_of(1, 0, core, late * HALF, HALF),
            z_send.at[1], z_recv.at[late], at(to_z, x, core),
        )

    def x_half(way, late):
        return remote(
            part_of(1, 0, core, late * HALF, HALF), part_of(1, 1 + way, core, late * HALF, HALF),
            x_send.at[1, way], x_recv.at[1, way], sides[way],
        )

    def first_copy(way, late):
        low = HALF * (way ^ late)
        return remote(
            part_of(0, 0, core, low, HALF), part_of(0, 1 + way, core, low, HALF),
            o_send.at[way, late], o_recv.at[way, late], sides[way],
        )

    def f_copy(k, way):
        return remote(
            part_of(k, 1 + way, core, way * HALF, HALF), part_of(k, 3, core, way * HALF, HALF),
            f_send.at[k, way], f_recv.at[k, way], sides[way],
        )

    def d_copy(k, piece, whose):
        if piece < 3:
            block = part_of(k, piece, whose)
        else:
            block = part_of(k, 3, whose, (piece - 3) * HALF, HALF)
        return remote(block, block, d_send.at[k, piece], d_recv.at[k, piece], partner)

    def pass_far(k):
        for way in range(2):
            f_copy(k, way).wait_recv()
            d_copy(k, 3 + way, core).start()

    def place_tails(k, low, rows, unfold):
        extra = rows // MAIN * tail
        room = -(-extra // 16) * 16
        folded = gathered[k, low:low + rows, features:features + width]
        plain = jnp.dot(unfold[...], folded, preferred_element_type=F32)
        for part in range(fold):
            piece = plain[part * extra:(part + 1) * extra]
            piece = jnp.concatenate([piece, jnp.zeros((room - extra, width), F32)], axis=0).astype(BF16)
            gathered[k, low + rows:low + rows + room, part * width:(part + 1) * width] = piece

    def multiply(k, low, rows, places, first, count):
        product = lax.dot_general(
            gathered[k, low:low + rows, 0:features], weight_t[:, first:first + count],
            (((1,), (0,)), ((), ())), preferred_element_type=F32,
        )
        size = jnp.max(jnp.abs(product).reshape(rows // 8, 8, count), axis=0)
        size = functools.reduce(jnp.maximum, [size[:, i:i + 128] for i in range(0, count, 128)])
        hidden_peak[...] = jnp.maximum(hidden_peak[...], size)
        result = jnp.clip(product * factor, -1.0, 1.0)
        from_z = (z + offset(k) + n_z) % n_z
        for place in places:
            start = starts[place] - low
            last = (NEAR + place * CORES * tail if place < 3 else FAR + PAIR) - low
            pieces = []
            for member in range(CORES):
                pieces.append(result[start + member * MAIN:start + (member + 1) * MAIN])
                pieces.append(result[last + member * tail:last + (member + 1) * tail])
            ordered = jnp.concatenate(pieces, axis=0).astype(BF16)
            out_ref[from_z * n_x + (x, left, right, far)[place], :, first:first + count] = ordered

    def near_ready(k):
        for piece in range(3):
            d_copy(k, piece, 1 - core).wait_recv()
        place_tails(k, 0, NEAR, unfold_near)

    def far_ready(k):
        for piece in range(3, 5):
            d_copy(k, piece, 1 - core).wait_recv()
        place_tails(k, FAR, PAIR, unfold_far)

    def send_own(k):
        x_copy(k, 0).start()
        x_copy(k, 1).start()
        d_copy(k, 0, core).start()

    def z_body(k, carry):
        z_copy(k).start()
        return carry

    for late in range(2):
        for way in range(2):
            first_copy(way, late).start()
    z_half(0).start()
    z_half(1).start()
    lax.fori_loop(2, n_z, z_body, 0)
    d_copy(0, 0, core).start()
    weight_in.wait()

    last = n_z - 1

    def transpose(block, carry):
        start = pl.multiple_of(block * TURNED, TURNED)
        weight_t[pl.ds(start, TURNED), :] = weight_v[:, pl.ds(start, TURNED)].T
        return carry

    blocks = features // TURNED
    early = blocks * EARLY // 12

    def step(i, carry):
        @pl.when(i < last)
        def _():
            z_copy(i + 1).wait_recv()
            send_own(i + 1)

        @pl.when(i == 1)
        def _():
            lax.fori_loop(early, blocks, transpose, 0)

        @pl.when(i >= 2)
        def _():
            k = i - 2
            pass_far(k)
            near_ready(k)
            far_ready(k)
            multiply(k, 0, FAR + FAR_ROWS, (0, 1, 2, 3), 0, units)

        for way in range(2):
            x_copy(i, way).wait_recv()
            f_copy(i, way).start()
            d_copy(i, 1 + way, core).start()
        return carry

    lax.fori_loop(0, early, transpose, 0)
    for way in range(2):
        first_copy(way, 0).wait_recv()
        f_copy(0, way).start()
    for late in range(2):
        z_half(late).wait_recv()
        x_half(0, late).start()
        x_half(1, late).start()
    d_copy(1, 0, core).start()
    for way in range(2):
        first_copy(way, 1).wait_recv()
        d_copy(0, 1 + way, core).start()
    lax.fori_loop(1, n_z, step, 0)
    near_ready(last)
    multiply(last, 0, FAR, (0, 1, 2), 0, units // 2)
    pass_far(last - 1)
    multiply(last, 0, FAR, (0, 1, 2), units // 2, units // 2)
    near_ready(last - 1)
    far_ready(last - 1)
    multiply(last - 1, 0, FAR + FAR_ROWS, (0, 1, 2, 3), 0, units // 2)
    pass_far(last)
    multiply(last - 1, 0, FAR + FAR_ROWS, (0, 1, 2, 3), units // 2, units // 2)
    far_ready(last)
    multiply(last, FAR, FAR_ROWS, (3,), 0, units)

    hidden_max = jnp.max(jnp.max(hidden_peak[...], axis=0, keepdims=True), axis=1, keepdims=True) / own_in
    hidden_row = jnp.where(iota((1, 128), 1) == z, hidden_max, 0.0)
    current = jnp.where(iota((2, 128), 0) == 0, peaks[...], hidden_row)
    others = n_y * members - 1
    chips = [(i, j) for i in range(n_y) for j in range(n_x)]

    def gather_copy(index):
        i, j = chips[index]
        hub = ((y + i) % n_y, (z * n_x + (x + j) % n_x) * CORES + 1)
        slot = others - (index * CORES + 1 - core)
        return remote(message.at[0], inbox.at[slot], m_send.at[index], m_recv.at[0], hub)

    def hub_copy(place, slot, peer, sem):
        return remote(message.at[1], inbox.at[others + 1 + slot], h_send.at[place], m_recv.at[sem], peer)

    def arrived(low, count, sem):
        block = inbox.at[pl.ds(low, count)]
        remote(block, block, m_send.at[0], m_recv.at[sem], partner).wait_recv()
        return jnp.max(inbox[low:low + count], axis=0)

    hub_copies = [hub_copy(to * (n_z - 1) + j, j, peers[1 + to][j], 1) for to in range(2) for j in range(n_z - 1)]
    hub_copies.append(hub_copy(2 * (n_z - 1), n_z - 1, partner, 2))
    message[0] = current
    for index in range(1, len(chips)):
        gather_copy(index).start()

    @pl.when(core == 0)
    def _():
        gather_copy(0).start()
        message[1] = arrived(others + n_z, 1, 2)

    @pl.when(core == 1)
    def _():
        message[1] = jnp.maximum(message[0], arrived(0, others, 0))
        for copy in hub_copies:
            copy.start()

    current = jnp.maximum(message[1], arrived(others + 1, n_z - 1, 1))

    new_grad[...] = jnp.concatenate([hist_grad[...][1:], current[0:1, 0:n_z]], axis=0)
    new_hidden[...] = jnp.concatenate([hist_hidden[...][1:], current[1:2, 0:n_z]], axis=0)

    def drain(k, carry):
        @pl.when(k >= 1)
        def _():
            z_copy(k).wait_send()
            x_copy(k, 0).wait_send()
            x_copy(k, 1).wait_send()

        for way in range(2):
            f_copy(k, way).wait_send()
        for piece in range(5):
            d_copy(k, piece, core).wait_send()
        return carry

    for way in range(2):
        for late in range(2):
            first_copy(way, late).wait_send()
    lax.fori_loop(0, n_z, drain, 0)
    for index in range(1, len(chips)):
        gather_copy(index).wait_send()

    @pl.when(core == 0)
    def _():
        gather_copy(0).wait_send()

    @pl.when(core == 1)
    def _():
        for copy in hub_copies:
            copy.wait_send()


def write_out(*refs):
    count = len(refs) // 2
    sems = refs[-1]
    copies = []
    for i in range(3):
        cuts = PIECES if i == 0 else 1
        size = refs[i].shape[0] // cuts
        for j in range(cuts):
            source, target = (ref.at[pl.ds(j * size, size)] for ref in (refs[i], refs[count + i]))
            copies.append(pltpu.make_async_copy(source, target, sems.at[len(copies)]))
    for copy in copies:
        copy.start()
    for copy in copies:
        copy.wait()


def solution(mesh):
    n_y = mesh.shape["dp"]
    n_expert = mesh.shape["expert"]

    def per_device(grad_out, expert_ids, down_weight, history_grad, history_hidden):
        tok, features = grad_out.shape
        n_z = history_grad.shape[1]
        members = n_expert // n_z
        n_x = members // CORES
        units = down_weight.shape[1]
        capacity = tok * 9 // 32
        width = features * (capacity - MAIN) // MAIN
        n_messages = n_y * members + n_z
        dma = pltpu.SemaphoreType.DMA
        anywhere = pl.BlockSpec(memory_space=pl.ANY)
        vmem, hbm = pl.BlockSpec(memory_space=pltpu.VMEM), pl.BlockSpec(memory_space=pltpu.HBM)
        small = jax.ShapeDtypeStruct(history_grad.shape, F32)
        arguments = expert_ids.T, history_grad, history_hidden, grad_out, down_weight[0]
        results = pl.pallas_call(
            functools.partial(kernel, n_y, n_z, n_x, capacity),
            out_shape=(jax.ShapeDtypeStruct((n_expert // CORES, CORES * capacity, units), BF16), small, small),
            in_specs=[hbm] * 5,
            out_specs=(vmem, vmem, vmem),
            scratch_shapes=[
                pltpu.VMEM((2, tok), jnp.int32),
                pltpu.VMEM(history_grad.shape, F32),
                pltpu.VMEM(history_grad.shape, F32),
                pltpu.VMEM((tok, features), BF16),
                pltpu.VMEM((units, features), BF16),
                pltpu.VMEM((features, units), BF16),
                pltpu.VMEM((n_z, MAIN, features + width), BF16),
                pltpu.VMEM((n_z, FAR + FAR_ROWS, features + width), BF16),
                pltpu.VMEM((n_z, tok), F32),
                pltpu.VMEM((NEAR, NEAR), BF16),
                pltpu.VMEM((PAIR, PAIR), BF16),
                pltpu.VMEM((1, 128), F32),
                pltpu.VMEM((8, 128), F32),
                pltpu.VMEM((2, 2, 128), F32),
                pltpu.VMEM((n_messages, 2, 128), F32),
                dma((5,)),
                dma((n_z,)), dma((n_z,)),
                dma((2, 2)), dma((2, 2)),
                dma((n_z, 2)), dma((n_z, 2)),
                dma((n_z, 2)), dma((n_z, 2)),
                dma((n_z, 5)), dma((n_z, 5)),
                dma((n_y * n_x,)), dma((3,)), dma((2 * n_z - 1,)),
            ],
            compiler_params=pltpu.CompilerParams(
                collective_id=0, has_side_effects=True, vmem_limit_bytes=46 * 1024 * 1024
            ),
        )(*(pltpu.with_memory_space_constraint(a, pltpu.HBM) for a in arguments))
        rows, new_grad, new_hidden = pl.pallas_call(
            write_out,
            out_shape=tuple(jax.ShapeDtypeStruct(a.shape, a.dtype) for a in results),
            in_specs=[anywhere] * 3,
            out_specs=(hbm,) * 3,
            scratch_shapes=[dma((PIECES + 2,))],
            compiler_params=pltpu.CompilerParams(vmem_limit_bytes=1024 * 1024),
        )(*results)
        return rows.reshape(1, 1, n_expert * capacity, units), new_grad, new_hidden

    both = ("dp", "expert")
    return jax.shard_map(
        per_device,
        mesh=mesh,
        in_specs=(P(both, None), P(both, None), P("expert", None, None), P(), P()),
        out_specs=(P("dp", "expert", None, None), P(), P()),
        check_vma=False,
    )
```
